32 devices in a mesh: row: 8 (over z, y), col: 4 (over x, core).
Axes of the slice: x: 2, y: 2, z: 4, core: 2. Of those that a mesh axis runs over, the one named last changes fastest.
Arguments:
- matrix: float32 [1536, 1536], P('row', 'col'), may hold values from -30 to 30
- panels: float32 [2, 1536, 256], P(None, ('col', 'row')), may hold values from -0.15625 to 0.15625
- factors: float32 [2, 256, 256], replicated, may hold values from -1 to 2, as said below
Outputs:
- reduced: float32 [1536, 1536], P('row', 'col')
The draws below stay inside these ranges and needn't reach their ends.
Inputs may be any that keep to these rules, and one draw needn't show every extreme that they name: Each factors[s] is upper triangular with diagonal entries between 1 and 2.
All inputs are finite; a program needn't handle non-finite values.
Results may differ from the reference program's by a relative error of at most 0.0003.
Values sent between devices are 32-bit elements; how exact they have to be, the bound alone decides.
No kernel may reach another device: no remote copies, remote signals or barrier semaphores. Data moves between devices by JAX's collectives and lax.ppermute only.
A program may use at most 64 MiB of HBM per device.

```python
import jax
import jax.numpy as jnp
from jax import lax

PANEL = 256
STEPS = 2
ORDER = 1536


def draw_matrix(key, part):
    first_key = jax.random.fold_in(jax.random.fold_in(key, 11), 0)
    noise = jax.random.truncated_normal(first_key, -5.0, 5.0, (ORDER, ORDER), jnp.float32)
    mirror = (noise + noise.T) * 0.5 ** 0.5
    return mirror


def draw_factors(key, part):
    first_key, second_key = jax.random.split(jax.random.fold_in(key, 23))
    diagonal = jax.random.uniform(first_key, (STEPS, PANEL), jnp.float32, 1.0, 2.0)
    spread = jax.random.truncated_normal(second_key, -4.0, 4.0, (STEPS, PANEL, PANEL), jnp.float32) * (0.5 * PANEL ** (-0.5))
    upper = jnp.triu(spread, 1)
    return upper + diagonal[:, :, None] * jnp.eye(PANEL, dtype=jnp.float32)[None, :, :]


def shard_levels(rng, extent, cuts, low, high):
    def one(position, blocks):
        steps = jax.random.uniform(jax.random.fold_in(jax.random.fold_in(rng, 6), position), (blocks,), jnp.float32, low / len(cuts), high / len(cuts))
        return jnp.repeat(jnp.exp(steps), extent[position] // blocks).reshape((-1,) + (1,) * (len(extent) - position - 1))

    level = one(*cuts[0])
    for cut in cuts[1:]:
        level = level * one(*cut)
    return level


def normal_values(rng, shape, deviation, reach, cuts=(), held_as=jnp.bfloat16):
    gain = shard_levels(rng, shape, cuts, -0.22, 0.18) if cuts else 1.0
    array = jax.random.normal(rng, shape, jnp.float32) * deviation * gain
    return jnp.minimum(jnp.maximum(array, -reach), reach).astype(held_as)


def setup_inputs(seed: int = 0) -> dict:
    key_of = jax.random.split(jax.random.key(seed), 4)
    return {
        "matrix": draw_matrix(jax.random.fold_in(key_of[3], 71), 0),
        "panels": normal_values(key_of[1], (STEPS, ORDER, PANEL), ORDER ** -0.5, 0.15625, ((1, 32),), jnp.float32),
        "factors": draw_factors(jax.random.fold_in(key_of[3], 71), 0),
    }


highest = lax.Precision.HIGHEST


def matmul(left, right):
    return jnp.dot(left, right, precision=highest, preferred_element_type=jnp.float32)


def reference(matrix, panels, factors):
    current = matrix
    for section in range(panels.shape[0]):
        panel = panels[section]
        factor = factors[section]
        image = matmul(matmul(current, panel), factor)
        inner = matmul(panel.T, image)
        update = image - 0.5 * matmul(panel, matmul(factor.T, inner))
        current = current - matmul(panel, update.T) - matmul(update, panel.T)
    return current
```

```python
import functools

import jax
import jax.numpy as jnp
from jax import lax
from jax.experimental import pallas as pl
from jax.experimental.pallas import tpu as pltpu
from jax.sharding import PartitionSpec as P

highest = lax.Precision.HIGHEST


def from_root(block, axis, owner):
    block = jnp.where(lax.axis_index(axis) == owner, block, jnp.zeros_like(block))
    return lax.psum(block, axis)


def matmul(left, right):
    return jnp.dot(left, right, precision=highest, preferred_element_type=jnp.float32)


def transposed_product(left, right):
    return lax.dot_general(
        left, right, (((0,), (0,)), ((), ())), precision=highest, preferred_element_type=jnp.float32
    )


def outer_product(left, right):
    return lax.dot_general(
        left, right, (((1,), (1,)), ((), ())), precision=highest, preferred_element_type=jnp.float32
    )


def general_device(matrix, panels, factors):
    row_count = lax.axis_size("row")
    col_count = lax.axis_size("col")
    my_row = lax.axis_index("row")
    block_rows = matrix.shape[0]
    share = panels.shape[1]
    source = my_row * col_count // row_count
    offset = share * (my_row * col_count - source * row_count)
    gathered = lax.all_gather(panels, "row", axis=1, tiled=True)
    relayed = from_root(gathered, "col", source)
    current = matrix
    for section in range(panels.shape[0]):
        factor = factors[section]
        panel_cols = gathered[section]
        panel_rows = lax.dynamic_slice_in_dim(relayed[section], offset, block_rows, 0)
        sums_rows = lax.psum(matmul(current, panel_cols), "col")
        sums_cols = lax.psum(transposed_product(current, panel_rows), "row")
        image_rows = matmul(sums_rows, factor)
        image_cols = matmul(sums_cols, factor)
        inner = lax.psum(transposed_product(panel_rows, image_rows), "row")
        correction = transposed_product(factor, inner)
        update_rows = image_rows - 0.5 * matmul(panel_rows, correction)
        update_cols = image_cols - 0.5 * matmul(panel_cols, correction)
        current = (
            current
            - outer_product(panel_rows, update_cols)
            - outer_product(update_rows, panel_cols)
        )
    return current


def split(value):
    high = value.astype(jnp.bfloat16)
    low = (value - high.astype(jnp.float32)).astype(jnp.bfloat16)
    return high, low


def dot3(left, right, dims=(1, 0)):
    numbers = (((dims[0],), (dims[1],)), ((), ()))
    one = functools.partial(
        lax.dot_general, dimension_numbers=numbers, preferred_element_type=jnp.float32
    )
    return one(left[0], right[0]) + (one(left[0], right[1]) + one(left[1], right[0]))


def place():
    row, col = lax.axis_index("row"), lax.axis_index("col")
    return row // 2, row % 2, col // 2, col % 2


def vmem(count):
    return [pl.BlockSpec(memory_space=pltpu.VMEM)] * count


def call(body, shapes, operands, scratch=(), flops=0):
    moved = sum(4 * o.size for o in operands) + sum(4 * s.size for s in shapes)
    return pl.pallas_call(
        body,
        out_shape=shapes,
        in_specs=vmem(len(operands)),
        out_specs=vmem(len(shapes)),
        scratch_shapes=list(scratch),
        cost_estimate=pl.CostEstimate(flops=flops, bytes_accessed=moved, transcendentals=0),
        compiler_params=pltpu.CompilerParams(vmem_limit_bytes=48 * 1024 * 1024),
    )(*operands)


def partial_body(depth, matrix_ref, *refs):
    slabs, out_ref, high, low = refs[: 2 * depth], refs[2 * depth], refs[-2], refs[-1]
    z, y, _, _ = place()
    share, width = slabs[0].shape[1], slabs[0].shape[2]
    for flip in range(2):
        for shift in range(depth):
            slab = slabs[flip * depth + shift]
            at = 2 * lax.rem(z - shift + depth, depth) + (1 - y if flip else y)
            rows = pl.ds(pl.multiple_of(at * share, share), share)
            for step in range(2):
                h, l = split(slab[step])
                high[rows, step * width : (step + 1) * width] = h
                low[rows, step * width : (step + 1) * width] = l
    out_ref[...] = dot3(split(matrix_ref[...]), (high[...], low[...]))


def panel_body(depth, *refs):
    slabs = refs[: 4 * depth]
    high_ref, low_ref, turned_high, turned_low, cross_ref, rows_ref, full = refs[4 * depth :]
    z, y, x, _ = place()
    share, width = slabs[0].shape[1], slabs[0].shape[2]
    column = 2 * depth * share
    for across in range(2):
        for flip in range(2):
            for shift in range(depth):
                slab = slabs[(2 * across + flip) * depth + shift]
                at = 2 * lax.rem(z - shift + depth, depth) + (1 - y if flip else y)
                start = (1 - x if across else x) * column + at * share
                rows = pl.ds(pl.multiple_of(start, share), share)
                for step in range(2):
                    full[rows, step * width : (step + 1) * width] = slab[step]
    high, low = split(full[...])
    high_ref[...], low_ref[...] = high, low
    turn_h, turn_l = split(full[...].T)
    turned_high[...], turned_low[...] = turn_h, turn_l
    first = (turn_h[:width], turn_l[:width])
    cross_ref[...] = dot3(first, (high[:, width:], low[:, width:]))
    block = 4 * share
    start = (z // 2) * column + y * block
    rows_ref[...] = full[pl.ds(pl.multiple_of(start, block), block), :]


def inner_body(depth, *refs):
    blocks = refs[:8]
    turned_high, turned_low, inner_ref, cols_ref, full = refs[8:]
    z, y, x, k = place()
    rows, width = blocks[0].shape[0], blocks[0].shape[1] // 2
    owner = z % 2 == k
    planes = (
        jnp.where(owner, z, lax.rem(z - 1 + depth, depth)),
        jnp.where(owner, lax.rem(z + 2, depth), lax.rem(z + 1, depth)),
    )
    for which in range(2):
        for flip in range(4):
            y_from = 1 - y if flip & 1 else y
            x_from = 1 - x if flip & 2 else x
            start = ((planes[which] // 2) * 4 + y_from * 2 + x_from) * rows
            full[pl.ds(pl.multiple_of(start, rows), rows), :] = blocks[4 * which + flip][...]
    high, low = split(full[...])
    first, second = slice(0, width), slice(width, 2 * width)
    for at, (v, p) in enumerate(((first, first), (second, first), (second, second))):
        inner_ref[at] = dot3((turned_high[v, :], turned_low[v, :]), (high[:, p], low[:, p]))
    cols_ref[...] = full[pl.ds(pl.multiple_of(x * 4 * rows, rows), 4 * rows), :]


def update_body(
    matrix_ref, factors_ref, inner_a, inner_b, cross_a, cross_b, high_ref, low_ref,
    panel_a, panel_b, cols_ref, near_a, far_a, near_b, far_b, out_ref, image, rows_v,
):
    z, y, x, k = place()
    owner = z % 2 == k
    width = factors_ref.shape[1]
    cols, half = cols_ref.shape[0], near_a.shape[0]
    image[pl.ds(0, cols), :] = cols_ref[...]
    near = pl.ds(pl.multiple_of(cols + x * half, half), half)
    far = pl.ds(pl.multiple_of(cols + (1 - x) * half, half), half)

    @pl.when(owner)
    def _():
        image[near, :] = near_a[...]
        image[far, :] = far_a[...]
        rows_v[...] = panel_a[...]

    @pl.when(jnp.logical_not(owner))
    def _():
        image[near, :] = near_b[...]
        image[far, :] = far_b[...]
        rows_v[...] = panel_b[...]

    factor1, factor2 = split(factors_ref[0]), split(factors_ref[1])
    g11 = split(inner_a[0] + inner_b[0])
    g21 = split(inner_a[1] + inner_b[1])
    g22 = inner_a[2] + inner_b[2]
    cross = split(cross_a[...] + cross_b[...])
    half_m1 = split(0.5 * dot3(factor1, split(dot3(g11, factor1)), (0, 0)))
    mixed = split(dot3(factor1, g21, (0, 1)) - dot3(half_m1, cross, (0, 0)))
    g22 = g22 - dot3(cross, mixed, (0, 0)) - dot3(mixed, cross, (0, 0))
    half_m2 = split(0.5 * dot3(factor2, split(dot3(split(g22), factor2)), (0, 0)))

    first, second = slice(0, width), slice(width, 2 * width)
    v_rows = split(rows_v[...])
    at = pl.ds(pl.multiple_of(x * cols, cols), cols)
    v_cols = (high_ref[at, :], low_ref[at, :])
    v_all = [jnp.concatenate([c, r], axis=0) for c, r in zip(v_cols, v_rows)]
    v1 = [v[:, first] for v in v_all]
    v2 = [v[:, second] for v in v_all]
    u1 = split(dot3(split(image[:, first]), factor1) - dot3(v1, half_m1))
    image2 = image[:, second] - dot3(v1, mixed) - dot3(u1, cross)
    u2 = split(dot3(split(image2), factor2) - dot3(v2, half_m2))

    total = matrix_ref[...]
    for v, u in ((v1, u1), (v2, u2)):
        top_v, top_u = [w[cols:] for w in v], [w[cols:] for w in u]
        side_v, side_u = [w[:cols] for w in v], [w[:cols] for w in u]
        total = total - dot3(top_v, side_u, (1, 1)) - dot3(top_u, side_v, (1, 1))
    out_ref[...] = total


def plane_device(matrix, panels, factors):
    row_count, col_count = lax.axis_size("row"), lax.axis_size("col")
    depth = row_count // 2
    z, y, x, k = place()
    owner = z % 2 == k
    f32 = jnp.float32

    def send(value, target, source=lambda z, y, x, k: True):
        pairs = []
        for index in range(row_count * col_count):
            row, col = divmod(index, col_count)
            at = (row // 2, row % 2, col // 2, col % 2)
            if source(*at):
                to = target(*at)
                pairs.append((index, (to[0] * 2 + to[1]) * col_count + to[2] * 2 + to[3]))
        return lax.ppermute(value, ("row", "col"), pairs)

    def owns(z, y, x, k):
        return z % 2 == k

    def along_z(shift):
        return lambda z, y, x, k: ((z + shift) % depth, y, x, k)

    def to_y(z, y, x, k):
        return z, 1 - y, x, k

    def to_x(z, y, x, k):
        return z, y, 1 - x, k

    def to_core(z, y, x, k):
        return z, y, x, 1 - k

    _, share, width = panels.shape
    block, cols = matrix.shape
    half = block // 2

    order = [2, 1] + list(range(3, depth))
    slabs = {0: panels}
    for shift in order:
        slabs[shift] = send(panels, along_z(shift))
    own = [slabs[s] for s in range(depth)]
    beside = {s: send(slabs[s], to_y) for s in [0] + order}
    beside = [beside[s] for s in range(depth)]
    across = {s: send(slabs[s], to_x) for s in [0] + order}
    across = [across[s] for s in range(depth)]

    partial = call(
        functools.partial(partial_body, depth),
        [jax.ShapeDtypeStruct((block, 2 * width), f32)],
        [matrix, *own, *beside],
        [pltpu.VMEM((cols, 2 * width), jnp.bfloat16)] * 2,
        flops=6 * block * cols * width * 2,
    )[0]
    chip = partial + send(partial, to_core)
    kept = lax.dynamic_slice_in_dim(chip, x * half, half, 0)
    given = lax.dynamic_slice_in_dim(chip, (1 - x) * half, half, 0)
    mine = kept + send(given, to_x, owns)

    opposite = [send(a, to_y) for a in across]
    channel = 2 * cols
    panel_high, panel_low, turned_high, turned_low, cross, panel_rows = call(
        functools.partial(panel_body, depth),
        [
            jax.ShapeDtypeStruct((channel, 2 * width), jnp.bfloat16),
            jax.ShapeDtypeStruct((channel, 2 * width), jnp.bfloat16),
            jax.ShapeDtypeStruct((2 * width, channel), jnp.bfloat16),
            jax.ShapeDtypeStruct((2 * width, channel), jnp.bfloat16),
            jax.ShapeDtypeStruct((width, width), f32),
            jax.ShapeDtypeStruct((block, 2 * width), f32),
        ],
        [*own, *beside, *across, *opposite],
        [pltpu.VMEM((channel, 2 * width), f32)],
        flops=6 * channel * width * width,
    )
    cross_other = send(cross, to_core)
    panel_rows_other = send(panel_rows, to_core)

    before = send(mine, along_z(1), owns)
    two = send(mine, along_z(2), owns)
    after = send(mine, along_z(depth - 1), owns)
    first = jnp.where(owner, mine, before)
    second = jnp.where(owner, two, after)

    def spread(value):
        y_value, x_value = send(value, to_y), send(value, to_x)
        low, high = x_value[: half // 2], y_value[half // 2 :]
        corner = jnp.concatenate([send(low, to_y), send(high, to_x)], axis=0)
        return [value, y_value, x_value, corner]

    first4 = spread(first)
    second4 = spread(second)
    near_other, far_other = send(first4[0], to_core), send(first4[2], to_core)
    inner, image_cols = call(
        functools.partial(inner_body, depth),
        [
            jax.ShapeDtypeStruct((3, width, width), f32),
            jax.ShapeDtypeStruct((cols, 2 * width), f32),
        ],
        [*first4, *second4, turned_high, turned_low],
        [pltpu.VMEM((channel, 2 * width), f32)],
        flops=18 * channel * width * width,
    )
    inner_other = send(inner, to_core)
    rows = cols + block
    return call(
        update_body,
        [jax.ShapeDtypeStruct((block, cols), f32)],
        [
            matrix, factors, inner, inner_other, cross, cross_other, panel_high, panel_low,
            panel_rows, panel_rows_other, image_cols,
            first4[0], first4[2], near_other, far_other,
        ],
        [pltpu.VMEM((rows, 2 * width), f32), pltpu.VMEM((block, 2 * width), f32)],
        flops=36 * rows * width * width,
    )[0]


def per_device(matrix, panels, factors):
    row_count, col_count = lax.axis_size("row"), lax.axis_size("col")
    planes = row_count == 2 * col_count and col_count == 4 and panels.shape[0] == 2
    return (plane_device if planes else general_device)(matrix, panels, factors)


def solution(mesh):
    return jax.shard_map(
        per_device,
        mesh=mesh,
        in_specs=(P("row", "col"), P(None, ("col", "row"), None), P()),
        out_specs=P("row", "col"),
        check_vma=False,
    )
```

```python
import functools

import jax
import jax.numpy as jnp
from jax import lax
from jax.experimental import pallas as pl
from jax.experimental.pallas import tpu as pltpu
from jax.sharding import PartitionSpec as P


highest = lax.Precision.HIGHEST


def from_root(block, axis, owner):
    block = jnp.where(lax.axis_index(axis) == owner, block, jnp.zeros_like(block))
    return lax.psum(block, axis)


def matmul(left, right):
    return jnp.dot(left, right, precision=highest, preferred_element_type=jnp.float32)


def transposed_product(left, right):
    return lax.dot_general(
        left, right, (((0,), (0,)), ((), ())), precision=highest, preferred_element_type=jnp.float32
    )


def outer_product(left, right):
    return lax.dot_general(
        left, right, (((1,), (1,)), ((), ())), precision=highest, preferred_element_type=jnp.float32
    )


def general_device(matrix, panels, factors):
    row_count = lax.axis_size("row")
    col_count = lax.axis_size("col")
    my_row = lax.axis_index("row")
    block_rows = matrix.shape[0]
    share = panels.shape[1]
    source = my_row * col_count // row_count
    offset = share * (my_row * col_count - source * row_count)
    gathered = lax.all_gather(panels, "row", axis=1, tiled=True)
    relayed = from_root(gathered, "col", source)
    current = matrix
    for section in range(panels.shape[0]):
        factor = factors[section]
        panel_cols = gathered[section]
        panel_rows = lax.dynamic_slice_in_dim(relayed[section], offset, block_rows, 0)
        sums_rows = lax.psum(matmul(current, panel_cols), "col")
        sums_cols = lax.psum(transposed_product(current, panel_rows), "row")
        image_rows = matmul(sums_rows, factor)
        image_cols = matmul(sums_cols, factor)
        inner = lax.psum(transposed_product(panel_rows, image_rows), "row")
        correction = transposed_product(factor, inner)
        update_rows = image_rows - 0.5 * matmul(panel_rows, correction)
        update_cols = image_cols - 0.5 * matmul(panel_cols, correction)
        current = (
            current
            - outer_product(panel_rows, update_cols)
            - outer_product(update_rows, panel_cols)
        )
    return current


def split(value):
    high = value.astype(jnp.bfloat16)
    low = (value - high.astype(jnp.float32)).astype(jnp.bfloat16)
    return high, low


def dot3(left, right, dims=(1, 0)):
    numbers = (((dims[0],), (dims[1],)), ((), ()))
    one = functools.partial(
        lax.dot_general, dimension_numbers=numbers, preferred_element_type=jnp.float32
    )
    return one(left[0], right[0]) + (one(left[0], right[1]) + one(left[1], right[0]))


def place():
    row, col = lax.axis_index("row"), lax.axis_index("col")
    return row // 2, row % 2, col // 2, col % 2


def vmem(count):
    return [pl.BlockSpec(memory_space=pltpu.VMEM)] * count


def call(body, shapes, operands, scratch=(), flops=0, space=pltpu.VMEM):
    moved = sum(4 * o.size for o in operands) + sum(4 * s.size for s in shapes)
    return pl.pallas_call(
        body,
        out_shape=shapes,
        in_specs=[pl.BlockSpec(memory_space=space)] * len(operands),
        out_specs=vmem(len(shapes)),
        scratch_shapes=list(scratch),
        cost_estimate=pl.CostEstimate(flops=flops, bytes_accessed=moved, transcendentals=0),
        compiler_params=pltpu.CompilerParams(vmem_limit_bytes=20 * 1024 * 1024),
    )(*operands)


def prepare_body(matrix_hbm, panels_hbm, factors_hbm, *refs):
    high_ref, low_ref, slab_ref, factor_high, factor_low, tile, factors, sems = refs
    copies = [
        pltpu.make_async_copy(matrix_hbm, tile, sems.at[0]),
        pltpu.make_async_copy(factors_hbm, factors, sems.at[1]),
        pltpu.make_async_copy(panels_hbm, slab_ref, sems.at[2]),
    ]
    for copy in copies:
        copy.start()
    copies[0].wait()
    high_ref[...], low_ref[...] = split(tile[...])
    copies[1].wait()
    factor_high[...], factor_low[...] = split(factors[...])
    copies[2].wait()


def partial_body(depth, high_a, low_a, factor_high, factor_low, *refs):
    slabs, (keep_ref, give_ref, high, low) = refs[: 2 * depth], refs[2 * depth :]
    z, y, x, k = place()
    share, width = slabs[0].shape[1], slabs[0].shape[2]
    for flip in range(2):
        for shift in range(depth):
            slab = slabs[flip * depth + shift]
            at = 2 * lax.rem(z - shift + depth, depth) + (1 - y if flip else y)
            rows = pl.ds(pl.multiple_of(at * share, share), share)
            for step in range(2):
                h, l = split(slab[step])
                high[rows, step * width : (step + 1) * width] = h
                low[rows, step * width : (step + 1) * width] = l
    product = dot3((high_a[...], low_a[...]), (high[...], low[...]))
    quarter = product.shape[0] // 4
    for step in range(2):
        factor = (factor_high[step], factor_low[step])
        image = dot3(split(product[:, step * width : (step + 1) * width]), factor)
        for h in range(2):
            for c in range(2):
                piece = image[(2 * h + c) * quarter : (2 * h + c + 1) * quarter]
                side = jnp.where(x == h, 0, 1)

                @pl.when(k == c)
                def _(piece=piece, side=side, step=step):
                    keep_ref[side, step] = piece

                @pl.when(k != c)
                def _(piece=piece, side=side, step=step):
                    give_ref[side, step] = piece


EARLY = ((0, 0), (0, 1), (0, 2), (1, 0))
LATE = ((0, 3), (1, 1), (1, 2), (1, 3))


def row_of(depth, which, flip, rows):
    z, y, x, k = place()
    other = jnp.where(z % 2 == k, lax.rem(z + 2, depth), lax.rem(z - 1 + depth, depth))
    near = jnp.where(z % 2 == k, z, lax.rem(z + 1, depth))
    plane = other if which else near
    y_from = 1 - y if flip & 1 else y
    x_from = 1 - x if flip & 2 else x
    return pl.multiple_of(((plane // 2) * 4 + y_from * 2 + x_from) * rows, rows)


def panel_body(depth, *refs):
    factor_high, factor_low, across_ref, opposite_ref = refs[:4]
    slabs = refs[4 : 4 + 2 * depth]
    turned_high, turned_low, high_ref, low_ref, cross_ref, rows_ref, full, turning = refs[4 + 2 * depth :]
    z, y, x, _ = place()
    share, width = slabs[0].shape[1], slabs[0].shape[2]
    column = 2 * depth * share
    for across in range(2):
        for flip in range(2):
            for shift in range(depth):
                if across:
                    slab = (opposite_ref if flip else across_ref).at[shift]
                else:
                    slab = slabs[flip * depth + shift]
                at = 2 * lax.rem(z - shift + depth, depth) + (1 - y if flip else y)
                start = (1 - x if across else x) * column + at * share
                rows = pl.ds(pl.multiple_of(start, share), share)
                for step in range(2):
                    full[rows, step * width : (step + 1) * width] = slab[step]
    half = 2 * share
    for at, (which, flip) in enumerate(EARLY + LATE):
        turning[at * half : (at + 1) * half, :] = full[pl.ds(row_of(depth, which, flip, half), half), :]
    first, second = split(turning[:, :width]), split(turning[:, width:])
    turned = (
        dot3((factor_high[0], factor_low[0]), first, (0, 1)),
        turning[:, width:].T,
        dot3((factor_high[1], factor_low[1]), second, (0, 1)),
    )
    for at, value in enumerate(turned):
        rows = slice(at * width, (at + 1) * width)
        turned_high[rows, :], turned_low[rows, :] = split(value)
    cross_ref[...] = dot3(first, second, (0, 0))
    block = 4 * share
    start = (z // 2) * column + y * block
    rows_ref[...] = full[pl.ds(pl.multiple_of(start, block), block), :]
    cols = pl.ds(pl.multiple_of(x * column, column), column)
    high_ref[...], low_ref[...] = split(full[cols, :])


def products(turned_high, turned_low, image, span):
    width = image.shape[1] // 2
    high, low = split(image[...])
    for at, p in enumerate((slice(0, width), slice(0, width), slice(width, 2 * width))):
        v = slice(at * width, (at + 1) * width)
        yield dot3((turned_high[v, span], turned_low[v, span]), (high[:, p], low[:, p]))


def fill(image, at, half, step, block):
    quarter, width = half.shape[-2], half.shape[-1]
    rows = pl.ds(at + block * quarter, quarter)
    image[rows, step * width : (step + 1) * width] = half[...]


def pieces(block):
    for step in range(2):
        part = block.at[step] if not isinstance(block, tuple) else block[step]
        for q in range(2):
            if isinstance(part, tuple):
                yield step, q, part[q]
            else:
                yield step, q, part.at[q]


def early_body(*refs):
    near, near_y, near_x, ahead0, ahead1, turned_high, turned_low, inner_ref, image = refs
    rows = image.shape[0] // 4
    for at, block in enumerate((near, near_y, near_x, (ahead0, ahead1))):
        for step, q, part in pieces(block):
            fill(image, at * rows, part, step, q)
    span = slice(0, 4 * rows)
    for at, value in enumerate(products(turned_high, turned_low, image, span)):
        inner_ref[at] = value


def late_body(*refs):
    (low, high, y0, y1, x0, x1, d1, before, turned_high, turned_low, inner_ref, image) = refs
    rows = image.shape[0] // 4
    near_d, ahead_d0 = split_corner(low, high)
    for at, block in enumerate((near_d, (y0, y1), (x0, x1), (ahead_d0, d1))):
        for step, q, part in pieces(block):
            fill(image, at * rows, part, step, q)
    span = slice(4 * rows, 8 * rows)
    for at, value in enumerate(products(turned_high, turned_low, image, span)):
        inner_ref[at] = before[at] + value


def split_corner(low, high):
    return ((low.at[0], high.at[0]), (low.at[1], high.at[1])), (low.at[2], high.at[2])


def base_body(depth, *refs):
    (
        matrix_ref, factor_high, factor_low, cross_a, cross_b, high_ref, low_ref, panel_a, panel_b,
        near, near_y, near_x, f0, f0y, f0x, f1, f1y, f1x, f1d, low, high, mine_ref, far_b,
        out_ref, rows_high, rows_low, cross_ref, full, image, rows_v,
    ) = refs
    z, _, x, k = place()
    owner = z % 2 == k
    width = cross_a.shape[0]
    quarter = near.shape[2]
    half, cols = 2 * quarter, high_ref.shape[0]
    near_d, f0d = split_corner(low, high)
    blocks = {
        (0, 0): near, (0, 1): near_y, (0, 2): near_x, (0, 3): near_d,
        (1, 0): (f0, f1), (1, 1): (f0y, f1y), (1, 2): (f0x, f1x), (1, 3): (f0d, f1d),
    }
    for (which, flip), block in blocks.items():
        for step, q, part in pieces(block):
            fill(full, row_of(depth, which, flip, half), part, step, q)
    image[pl.ds(0, cols), :] = full[pl.ds(pl.multiple_of(x * cols, cols), cols), :]
    for step, q, part in pieces(mine_ref):
        fill(image, pl.multiple_of(cols + x * half, half), part, step, q)
    far = pl.multiple_of(cols + (1 - x) * half, half)

    @pl.when(owner)
    def _():
        for step, q, part in pieces(near_x):
            fill(image, far, part, step, q)
        rows_v[...] = panel_a[...]

    @pl.when(jnp.logical_not(owner))
    def _():
        for step, q, part in pieces(far_b):
            fill(image, far, part, step, q)
        rows_v[...] = panel_b[...]

    cross = cross_a[...] + cross_b[...]
    cross_f = dot3(split(cross), (factor_high[1], factor_low[1]))
    cross_ref[0], cross_ref[1] = cross, cross_f
    first, second = slice(0, width), slice(width, 2 * width)
    w1 = split(image[:, first])
    w2 = split(image[:, second] - dot3(w1, split(cross_f)))
    v_rows = split(rows_v[...])
    rows_high[...], rows_low[...] = v_rows
    total = matrix_ref[...]
    for w, at in ((w1, first), (w2, second)):
        v_side = (high_ref[:, at], low_ref[:, at])
        v_top = [v[:, at] for v in v_rows]
        total = total - dot3(v_top, [p[:cols] for p in w], (1, 1))
        total = total - dot3([p[cols:] for p in w], v_side, (1, 1))
    out_ref[...] = total


def update_body(
    base_ref, factor_high, factor_low, inner_a, inner_b, cross_ref,
    high_ref, low_ref, rows_high, rows_low, out_ref,
):
    width = cross_ref.shape[1]
    first, second = slice(0, width), slice(width, 2 * width)
    factor2 = (factor_high[1], factor_low[1])
    cross, cross_f = split(cross_ref[0]), split(cross_ref[1])
    m1 = 0.5 * (inner_a[0] + inner_b[0])
    m1_split = split(m1)
    v1 = (rows_high[:, first], rows_low[:, first])
    v2 = (rows_high[:, second], rows_low[:, second])
    mixed_t = split(inner_a[1] + inner_b[1] - dot3(cross, m1_split, (0, 0)))
    mixed_f = dot3(mixed_t, factor2, (0, 0))
    twice = dot3(cross_f, split(mixed_f), (0, 0))
    side = mixed_f - dot3(m1_split, cross_f)
    m2 = 0.5 * (inner_a[2] + inner_b[2] - twice - twice.T)
    side_split = split(side)
    left = dot3(v1, split(m1 + m1.T)) + dot3(v2, side_split, (1, 1))
    right = dot3(v1, side_split) + dot3(v2, split(m2 + m2.T))
    out_ref[...] = (
        base_ref[...]
        + dot3(split(left), (high_ref[:, first], low_ref[:, first]), (1, 1))
        + dot3(split(right), (high_ref[:, second], low_ref[:, second]), (1, 1))
    )


def plane_device(matrix, panels, factors):
    row_count, col_count = lax.axis_size("row"), lax.axis_size("col")
    depth = row_count // 2
    z, _, _, k = place()
    owner = z % 2 == k
    f32, bf16 = jnp.float32, jnp.bfloat16
    shape = jax.ShapeDtypeStruct

    def send(value, target):
        pairs = []
        for index in range(row_count * col_count):
            row, col = divmod(index, col_count)
            to = target(row // 2, row % 2, col // 2, col % 2)
            pairs.append((index, (to[0] * 2 + to[1]) * col_count + to[2] * 2 + to[3]))
        return lax.ppermute(value, ("row", "col"), pairs)

    def along_z(shift):
        return lambda z, y, x, k: ((z + shift) % depth, y, x, k)

    def to_y(z, y, x, k):
        return z, 1 - y, x, k

    def to_x(z, y, x, k):
        return z, y, 1 - x, k

    def to_corner(z, y, x, k):
        return z, 1 - y, 1 - x, k

    def to_core(z, y, x, k):
        return z, y, x, 1 - k

    def forward(z, y, x, k):
        return ((z + (2 if k == z % 2 else 1)) % depth, y, x, z % 2)

    def backward(z, y, x, k):
        return ((z - 1) % depth if k == z % 2 else z, y, x, z % 2)

    _, _, width = panels.shape
    block, cols = matrix.shape
    quarter, channel = block // 4, 2 * cols

    high_a, low_a, slab, factor_high, factor_low = call(
        prepare_body,
        [
            shape(matrix.shape, bf16), shape(matrix.shape, bf16), shape(panels.shape, f32),
            shape(factors.shape, bf16), shape(factors.shape, bf16),
        ],
        [matrix, panels, factors],
        [
            pltpu.VMEM(matrix.shape, f32), pltpu.VMEM(factors.shape, f32),
            pltpu.SemaphoreType.DMA((3,)),
        ],
        space=pltpu.HBM,
    )

    order = [2, 1] + list(range(3, depth))
    slabs = {0: slab}
    for shift in order:
        slabs[shift] = send(panels, along_z(shift))
    own = [slabs[s] for s in range(depth)]
    beside = [send(slabs[s], to_y) for s in range(depth)]
    across = [send(slabs[s], to_x) for s in range(depth)]

    keep, give = call(
        functools.partial(partial_body, depth),
        [shape((2, 2, quarter, width), f32)] * 2,
        [high_a, low_a, factor_high, factor_low, *own, *beside],
        [pltpu.VMEM((cols, 2 * width), bf16)] * 2,
        flops=6 * block * cols * width * 2,
    )
    chip = keep + send(give, to_core)
    piece = chip[0] + send(chip[1], to_x)
    other = send(piece, to_core)
    mine = jnp.where(k == 0, jnp.stack([piece, other], axis=1), jnp.stack([other, piece], axis=1))

    stacked = jnp.stack(across)
    opposite = send(stacked, to_y)
    turned_high, turned_low, panel_high, panel_low, cross, panel_rows = call(
        functools.partial(panel_body, depth),
        [
            shape((3 * width, channel), bf16),
            shape((3 * width, channel), bf16),
            shape((cols, 2 * width), bf16),
            shape((cols, 2 * width), bf16),
            shape((width, width), f32),
            shape((block, 2 * width), f32),
        ],
        [factor_high, factor_low, stacked, opposite, *own, *beside],
        [pltpu.VMEM((channel, 2 * width), f32)] * 2,
        flops=6 * channel * width * width * 3,
    )
    cross_other = send(cross, to_core)
    panel_rows_other = send(panel_rows, to_core)

    near = jnp.where(owner, mine, send(mine, backward))
    ahead = [send(mine[step], forward) for step in range(2)]
    near_y, near_x = send(near, to_y), send(near, to_x)
    f0, f1 = ahead
    f0y, f0x = send(f0, to_y), send(f0, to_x)
    f1y, f1x, f1d = send(f1, to_y), send(f1, to_x), send(f1, to_corner)
    low = jnp.stack([near_x[0, 0], near_x[1, 0], f0x[0]])
    high = jnp.stack([near_y[0, 1], near_y[1, 1], f0y[1]])
    low, high = send(low, to_y), send(high, to_x)
    far_other = send(near_x, to_core)

    inner = call(
        early_body,
        [shape((3, width, width), f32)],
        [near, near_y, near_x, f0, f1, turned_high, turned_low],
        [pltpu.VMEM((cols, 2 * width), f32)],
        flops=9 * channel * width * width,
    )[0]
    inner = call(
        late_body,
        [shape((3, width, width), f32)],
        [low, high, f0y, f1y, f0x, f1x, f1d, inner, turned_high, turned_low],
        [pltpu.VMEM((cols, 2 * width), f32)],
        flops=9 * channel * width * width,
    )[0]
    inner_other = send(inner, to_core)
    rows = cols + block
    base, rows_high, rows_low, crosses = call(
        functools.partial(base_body, depth),
        [
            shape((block, cols), f32), shape((block, 2 * width), bf16),
            shape((block, 2 * width), bf16), shape((2, width, width), f32),
        ],
        [
            matrix, factor_high, factor_low, cross, cross_other, panel_high, panel_low,
            panel_rows, panel_rows_other, near, near_y, near_x, f0, f0y, f0x, f1, f1y, f1x, f1d,
            low, high, mine, far_other,
        ],
        [
            pltpu.VMEM((channel, 2 * width), f32), pltpu.VMEM((rows, 2 * width), f32),
            pltpu.VMEM((block, 2 * width), f32),
        ],
        flops=18 * rows * width * width,
    )
    return call(
        update_body,
        [shape((block, cols), f32)],
        [
            base, factor_high, factor_low, inner, inner_other, crosses,
            panel_high, panel_low, rows_high, rows_low,
        ],
        flops=18 * rows * width * width,
    )[0]


def per_device(planes, matrix, panels, factors):
    if not planes:
        return general_device(matrix, panels, factors)
    return plane_device(matrix, panels, factors)


def solution(mesh):
    row_count, col_count = mesh.shape["row"], mesh.shape["col"]
    planes = row_count == 2 * col_count and col_count == 4
    return jax.shard_map(
        functools.partial(per_device, planes),
        mesh=mesh,
        in_specs=(P("row", "col"), P(None, ("col", "row"), None), P()),
        out_specs=P("row", "col"),
        check_vma=False,
    )
```

```python
import functools

import jax
import jax.numpy as jnp
from jax import lax
from jax.experimental import pallas as pl
from jax.experimental.pallas import tpu as pltpu
from jax.sharding import PartitionSpec as P


highest = lax.Precision.HIGHEST


def from_root(block, axis, owner):
    block = jnp.where(lax.axis_index(axis) == owner, block, jnp.zeros_like(block))
    return lax.psum(block, axis)


def matmul(left, right):
    return jnp.dot(left, right, precision=highest, preferred_element_type=jnp.float32)


def transposed_product(left, right):
    return lax.dot_general(
        left, right, (((0,), (0,)), ((), ())), precision=highest, preferred_element_type=jnp.float32
    )


def outer_product(left, right):
    return lax.dot_general(
        left, right, (((1,), (1,)), ((), ())), precision=highest, preferred_element_type=jnp.float32
    )


def general_device(matrix, panels, factors):
    row_count = lax.axis_size("row")
    col_count = lax.axis_size("col")
    my_row = lax.axis_index("row")
    block_rows = matrix.shape[0]
    share = panels.shape[1]
    source = my_row * col_count // row_count
    offset = share * (my_row * col_count - source * row_count)
    gathered = lax.all_gather(panels, "row", axis=1, tiled=True)
    relayed = from_root(gathered, "col", source)
    current = matrix
    for section in range(panels.shape[0]):
        factor = factors[section]
        panel_cols = gathered[section]
        panel_rows = lax.dynamic_slice_in_dim(relayed[section], offset, block_rows, 0)
        sums_rows = lax.psum(matmul(current, panel_cols), "col")
        sums_cols = lax.psum(transposed_product(current, panel_rows), "row")
        image_rows = matmul(sums_rows, factor)
        image_cols = matmul(sums_cols, factor)
        inner = lax.psum(transposed_product(panel_rows, image_rows), "row")
        correction = transposed_product(factor, inner)
        update_rows = image_rows - 0.5 * matmul(panel_rows, correction)
        update_cols = image_cols - 0.5 * matmul(panel_cols, correction)
        current = (
            current
            - outer_product(panel_rows, update_cols)
            - outer_product(update_rows, panel_cols)
        )
    return current


def apart3(left, right, dims=(1, 0)):
    numbers = (((dims[0],), (dims[1],)), ((), ()))
    one = functools.partial(
        lax.dot_general, dimension_numbers=numbers, preferred_element_type=jnp.float32
    )
    return one(left[0], right[0]) + (one(left[0], right[1]) + one(left[1], right[0]))


def split(value):
    high = value.astype(jnp.bfloat16)
    low = (value - high.astype(jnp.float32)).astype(jnp.bfloat16)
    return high, low


def dot3(left, right, dims=(1, 0)):
    joined_left = jnp.concatenate([left[0], left[0], left[1]], axis=dims[0])
    joined_right = jnp.concatenate([right[0], right[1], right[0]], axis=dims[1])
    numbers = (((dims[0],), (dims[1],)), ((), ()))
    return lax.dot_general(
        joined_left, joined_right, numbers, preferred_element_type=jnp.float32
    )


def place():
    row, col = lax.axis_index("row"), lax.axis_index("col")
    return row // 2, row % 2, col // 2, col % 2


def vmem(count):
    return [pl.BlockSpec(memory_space=pltpu.VMEM)] * count


def call(body, shapes, operands, scratch=(), flops=0, space=pltpu.VMEM):
    moved = sum(4 * o.size for o in operands) + sum(4 * s.size for s in shapes)
    return pl.pallas_call(
        body,
        out_shape=shapes,
        in_specs=[pl.BlockSpec(memory_space=space)] * len(operands),
        out_specs=vmem(len(shapes)),
        scratch_shapes=list(scratch),
        cost_estimate=pl.CostEstimate(flops=flops, bytes_accessed=moved, transcendentals=0),
        compiler_params=pltpu.CompilerParams(vmem_limit_bytes=20 * 1024 * 1024),
    )(*operands)


def prepare_body(matrix_hbm, panels_hbm, factors_hbm, *refs):
    high_ref, low_ref, slab_ref, factor_high, factor_low, tile, factors, sems = refs
    copies = [
        pltpu.make_async_copy(matrix_hbm, tile, sems.at[0]),
        pltpu.make_async_copy(factors_hbm, factors, sems.at[1]),
        pltpu.make_async_copy(panels_hbm, slab_ref, sems.at[2]),
    ]
    for copy in copies:
        copy.start()
    copies[0].wait()
    high_ref[...], low_ref[...] = split(tile[...])
    copies[1].wait()
    factor_high[...], factor_low[...] = split(factors[...])
    copies[2].wait()


def share_of(core, high_a, low_a, panel, factor_high, factor_low, out_ref):
    _, _, x, _ = place()
    _, _, quarter, width = out_ref.shape
    rows = [
        pl.ds(pl.multiple_of((2 * h + core) * quarter, quarter), quarter) for h in (x, 1 - x)
    ]
    tile = [jnp.concatenate([a[r, :] for r in rows], axis=0) for a in (high_a, low_a)]
    product = dot3(tile, panel)
    for step in range(2):
        factor = (factor_high[step], factor_low[step])
        image = dot3(split(product[:, step * width : (step + 1) * width]), factor)
        for side in range(2):
            out_ref[side, step] = image[side * quarter : (side + 1) * quarter]


def give_body(depth, high_a, low_a, factor_high, factor_low, *refs):
    slabs, (give_ref, high, low) = refs[: 2 * depth], refs[2 * depth :]
    z, y, _, k = place()
    share, width = slabs[0].shape[1], slabs[0].shape[2]
    for flip in range(2):
        for shift in range(depth):
            slab = slabs[flip * depth + shift]
            at = 2 * lax.rem(z - shift + depth, depth) + (1 - y if flip else y)
            rows = pl.ds(pl.multiple_of(at * share, share), share)
            for step in range(2):
                h, l = split(slab[step])
                high[rows, step * width : (step + 1) * width] = h
                low[rows, step * width : (step + 1) * width] = l
    panel = (high[...], low[...])
    share_of(1 - k, high_a, low_a, panel, factor_high, factor_low, give_ref)


def keep_body(high_a, low_a, factor_high, factor_low, high, low, keep_ref):
    _, _, _, k = place()
    share_of(k, high_a, low_a, (high[...], low[...]), factor_high, factor_low, keep_ref)


EARLY = (("a", 0), ("b", 0), ("a", 1), ("b", 1), ("a", 2), ("b", 2), ("f", 0), ("f", 1))
LATE = (("a", 3), ("b", 3), ("f", 2), ("f", 3), ("g", 0), ("g", 1), ("g", 2), ("g", 3))


def row_of(depth, kind, flip, quarter):
    z, y, x, k = place()
    owner = z % 2 == k
    if kind in "ab":
        plane = jnp.where(owner, z, lax.rem(z + 1, depth))
    else:
        plane = jnp.where(owner, lax.rem(z + 2, depth), lax.rem(z - 1 + depth, depth))
    core = {"a": k, "b": 1 - k, "f": z % 2, "g": 1 - z % 2}[kind]
    y_from = 1 - y if flip & 1 else y
    x_from = 1 - x if flip & 2 else x
    block = (plane // 2) * 4 + y_from * 2 + x_from
    return pl.multiple_of((2 * block + core) * quarter, quarter)


def fill(image, start, parts):
    for step, part in enumerate(parts):
        quarter, width = part.shape
        image[pl.ds(start, quarter), step * width : (step + 1) * width] = part[...]


def steps(ref):
    return ref.at[0], ref.at[1]


def near_pieces(flip, ref):
    return {("a", flip): steps(ref.at[0]), ("b", flip): steps(ref.at[1])}


def corner_pieces(low, high):
    return {
        ("a", 3): (low.at[0], low.at[1]),
        ("b", 3): (high.at[0], high.at[1]),
        ("f", 3): (low.at[2], high.at[2]),
    }


def panel_body(depth, *refs):
    factor_high, factor_low, across_ref, opposite_ref = refs[:4]
    slabs = refs[4 : 4 + 2 * depth]
    (
        turn1_high, turn1_low, turn2_ref, turn3_high, turn3_low, cross_ref, rows_ref,
         full, turning,
    ) = refs[4 + 2 * depth :]
    z, y, x, _ = place()
    share, width = slabs[0].shape[1], slabs[0].shape[2]
    column = 2 * depth * share
    for across in range(2):
        for flip in range(2):
            for shift in range(depth):
                if across:
                    slab = (opposite_ref if flip else across_ref).at[shift]
                else:
                    slab = slabs[flip * depth + shift]
                at = 2 * lax.rem(z - shift + depth, depth) + (1 - y if flip else y)
                start = (1 - x if across else x) * column + at * share
                fill(full, pl.multiple_of(start, share), steps(slab))
    for at, (kind, flip) in enumerate(EARLY + LATE):
        rows = pl.ds(row_of(depth, kind, flip, share), share)
        turning[at * share : (at + 1) * share, :] = full[rows, :]
    first, second = split(turning[:, :width]), split(turning[:, width:])
    turn1_high[...], turn1_low[...] = split(
        0.5 * dot3((factor_high[0], factor_low[0]), first, (0, 1))
    )
    turn2 = dot3((factor_high[1], factor_low[1]), second, (0, 1))
    turn2_ref[...] = turn2
    turn3_high[...], turn3_low[...] = split(0.5 * turn2)
    cross_ref[...] = dot3(first, second, (0, 0))
    block = 4 * share
    start = (z // 2) * column + y * block
    rows_ref[...] = full[pl.ds(pl.multiple_of(start, block), block), :]


def cross_body(
    factor_high, factor_low, cross_a, cross_b, turn1_high, turn1_low, turn2_ref,
    mixed_high, mixed_low, out_high, out_low,
):
    cross = split(dot3(split(cross_a[...] + cross_b[...]), (factor_high[1], factor_low[1])))
    mixed_high[...], mixed_low[...] = cross
    turned = turn2_ref[...] - dot3(cross, (turn1_high[...], turn1_low[...]), (0, 0))
    out_high[...], out_low[...] = split(turned)


def products(turned, image, span):
    width = image.shape[1] // 2
    high, low = split(image[...])
    for (turn_high, turn_low), p in zip(turned, (0, 0, width)):
        side = slice(p, p + width)
        yield dot3((turn_high[:, span], turn_low[:, span]), (high[:, side], low[:, side]))


def early_body(near, near_y, near_x, f_own, f_y, *refs):
    turned, (inner_ref, image) = refs[:6], refs[6:]
    held = {("f", 0): steps(f_own), ("f", 1): steps(f_y)}
    for flip, ref in enumerate((near, near_y, near_x)):
        held.update(near_pieces(flip, ref))
    quarter = near.shape[2]
    for at, key in enumerate(EARLY):
        fill(image, at * quarter, held[key])
    pairs = (turned[0:2], turned[2:4], turned[4:6])
    for at, value in enumerate(products(pairs, image, slice(0, image.shape[0]))):
        inner_ref[at] = value


def late_body(low, high, f_x, g_own, g_y, g_x, g_d, before, *refs):
    turned, (inner_ref, image) = refs[:6], refs[6:]
    held = {("f", 2): steps(f_x), **corner_pieces(low, high)}
    for flip, ref in enumerate((g_own, g_y, g_x, g_d)):
        held["g", flip] = steps(ref)
    quarter = low.shape[1]
    for at, key in enumerate(LATE):
        fill(image, at * quarter, held[key])
    pairs = (turned[0:2], turned[2:4], turned[4:6])
    span = slice(image.shape[0], 2 * image.shape[0])
    for at, value in enumerate(products(pairs, image, span)):
        inner_ref[at] = before[at] + value


def base_body(depth, *refs):
    (
        matrix_ref, cross_high, cross_low, high_ref, low_ref, panel_a, panel_b,
        near, near_y, near_x, f_own, f_y, f_x, g_own, g_y, g_x, g_d, low, high,
        piece_a, piece_b, far_b, out_ref, rows_high, rows_low, full, image, rows_v,
    ) = refs
    z, _, x, k = place()
    owner = z % 2 == k
    quarter, width = low.shape[1], low.shape[2]
    cols = high_ref.shape[0]
    held = {("f", 0): steps(f_own), ("f", 1): steps(f_y), ("f", 2): steps(f_x)}
    held.update(corner_pieces(low, high))
    for flip, ref in enumerate((near, near_y, near_x)):
        held.update(near_pieces(flip, ref))
    for flip, ref in enumerate((g_own, g_y, g_x, g_d)):
        held["g", flip] = steps(ref)
    for (kind, flip), parts in held.items():
        fill(full, row_of(depth, kind, flip, quarter), parts)
    image[pl.ds(0, cols), :] = full[pl.ds(pl.multiple_of(x * cols, cols), cols), :]

    def row(side, core):
        return pl.multiple_of(cols + (2 * side + core) * quarter, quarter)

    fill(image, row(x, k), steps(piece_a))
    fill(image, row(x, 1 - k), steps(piece_b))

    @pl.when(owner)
    def _():
        for at, core in enumerate((k, 1 - k)):
            fill(image, row(1 - x, core), steps(near_x.at[at]))
        rows_v[...] = panel_a[...]

    @pl.when(jnp.logical_not(owner))
    def _():
        for at, core in enumerate((1 - k, k)):
            fill(image, row(1 - x, core), steps(far_b.at[at]))
        rows_v[...] = panel_b[...]

    first, second = slice(0, width), slice(width, 2 * width)
    w1 = split(image[:, first])
    w2 = split(image[:, second] - dot3(w1, (cross_high[...], cross_low[...])))
    v_rows = split(rows_v[...])
    rows_high[...], rows_low[...] = v_rows
    total = matrix_ref[...]
    for w, at in ((w1, first), (w2, second)):
        v_side = (high_ref[:, at], low_ref[:, at])
        v_top = [v[:, at] for v in v_rows]
        total = total - dot3(v_top, [p[:cols] for p in w], (1, 1))
        total = total - dot3([p[cols:] for p in w], v_side, (1, 1))
    out_ref[...] = total


def update_body(
    base_ref, inner_a, inner_b, cross_high, cross_low, high_ref, low_ref, rows_high, rows_low,
    out_ref,
):
    width = cross_high.shape[0]
    first, second = slice(0, width), slice(width, 2 * width)
    cross = (cross_high[...], cross_low[...])
    v1 = (rows_high[:, first], rows_low[:, first])
    v2 = (rows_high[:, second], rows_low[:, second])
    m1 = inner_a[0] + inner_b[0]
    mixed_t = inner_a[1] + inner_b[1]
    m2 = inner_a[2] + inner_b[2]
    m2 = m2 - apart3(split(mixed_t), cross)
    side = split(mixed_t.T - apart3(split(m1), cross))
    left = apart3(v1, split(m1 + m1.T)) + apart3(v2, side, (1, 1))
    right = apart3(v1, side) + apart3(v2, split(m2 + m2.T))
    out_ref[...] = (
        base_ref[...]
        + apart3(split(left), (high_ref[:, first], low_ref[:, first]), (1, 1))
        + apart3(split(right), (high_ref[:, second], low_ref[:, second]), (1, 1))
    )


def plane_device(matrix, panels, factors):
    row_count, col_count = lax.axis_size("row"), lax.axis_size("col")
    depth = row_count // 2
    z, _, _, k = place()
    owner = z % 2 == k
    f32, bf16 = jnp.float32, jnp.bfloat16
    shape = jax.ShapeDtypeStruct

    def send(value, target):
        pairs = []
        for index in range(row_count * col_count):
            row, col = divmod(index, col_count)
            to = target(row // 2, row % 2, col // 2, col % 2)
            pairs.append((index, (to[0] * 2 + to[1]) * col_count + to[2] * 2 + to[3]))
        return lax.ppermute(value, ("row", "col"), pairs)

    def along_z(shift):
        return lambda z, y, x, k: ((z + shift) % depth, y, x, k)

    def to_y(z, y, x, k):
        return z, 1 - y, x, k

    def to_x(z, y, x, k):
        return z, y, 1 - x, k

    def to_corner(z, y, x, k):
        return z, 1 - y, 1 - x, k

    def to_core(z, y, x, k):
        return z, y, x, 1 - k

    def ahead_first(z, y, x, k):
        return (z + (2 if k == z % 2 else 1)) % depth, y, x, z % 2

    def ahead_second(z, y, x, k):
        return (z + (1 if k == z % 2 else 2)) % depth, y, x, z % 2

    def back_first(z, y, x, k):
        return (z - 1) % depth if k == z % 2 else z, y, x, z % 2

    def back_second(z, y, x, k):
        return (z, y, 1 - x, k) if k == z % 2 else ((z - 1) % depth, y, x, z % 2)

    _, _, width = panels.shape
    block, cols = matrix.shape
    quarter, channel = block // 4, 2 * cols

    high_a, low_a, slab, factor_high, factor_low = call(
        prepare_body,
        [
            shape(matrix.shape, bf16), shape(matrix.shape, bf16), shape(panels.shape, f32),
            shape(factors.shape, bf16), shape(factors.shape, bf16),
        ],
        [matrix, panels, factors],
        [
            pltpu.VMEM(matrix.shape, f32), pltpu.VMEM(factors.shape, f32),
            pltpu.SemaphoreType.DMA((3,)),
        ],
        space=pltpu.HBM,
    )

    order = [2, 1] + list(range(3, depth))
    slabs = {0: slab}
    for shift in order:
        slabs[shift] = send(panels, along_z(shift))
    own = [slabs[s] for s in range(depth)]
    beside = [send(slabs[s], to_y) for s in range(depth)]
    across = [send(slabs[s], to_x) for s in range(depth)]

    share_shape, cols_shape = shape((2, 2, quarter, width), f32), shape((cols, 2 * width), bf16)
    held = [high_a, low_a, factor_high, factor_low]
    give, panel_high, panel_low = call(
        functools.partial(give_body, depth),
        [share_shape, cols_shape, cols_shape],
        [*held, *own, *beside],
        flops=3 * block * cols * width * 2,
    )
    keep = call(
        keep_body, [share_shape], [*held, panel_high, panel_low], flops=3 * block * cols * width * 2
    )[0]
    chip = keep + send(give, to_core)
    piece = chip[0] + send(chip[1], to_x)

    stacked = jnp.stack(across)
    opposite = send(stacked, to_y)
    turn1_high, turn1_low, turn2, turn3_high, turn3_low, cross, panel_rows = call(
        functools.partial(panel_body, depth),
        [
            *[shape((width, channel), bf16)] * 2,
            shape((width, channel), f32),
            *[shape((width, channel), bf16)] * 2,
            shape((width, width), f32),
            shape((block, 2 * width), f32),
        ],
        [factor_high, factor_low, stacked, opposite, *own, *beside],
        [pltpu.VMEM((channel, 2 * width), f32)] * 2,
        flops=6 * channel * width * width * 3,
    )
    cross_other = send(cross, to_core)
    cross_high, cross_low, turn2_high, turn2_low = call(
        cross_body,
        [*[shape((width, width), bf16)] * 2, *[shape((width, channel), bf16)] * 2],
        [factor_high, factor_low, cross, cross_other, turn1_high, turn1_low, turn2],
        flops=6 * channel * width * width,
    )
    turned = [turn1_high, turn1_low, turn2_high, turn2_low, turn3_high, turn3_low]
    panel_rows_other = send(panel_rows, to_core)

    back1, back2 = send(piece, back_first), send(piece, back_second)
    f_own, g_own = send(piece, ahead_first), send(piece, ahead_second)
    near = jnp.where(owner, jnp.stack([piece, back1]), jnp.stack([back1, back2]))
    near_y, near_x = send(near, to_y), send(near, to_x)
    f_y, f_x = send(f_own, to_y), send(f_own, to_x)
    g_y, g_x = send(g_own, to_y), send(g_own, to_x)
    g_d = send(g_own, to_corner)
    low = jnp.concatenate([near_x[0], f_x[:1]])
    high = jnp.concatenate([near_y[1], f_y[1:]])
    low, high = send(low, to_y), send(high, to_x)
    piece_other = send(piece, to_core)
    far_other = send(near_x, to_core)

    inner = call(
        early_body,
        [shape((3, width, width), f32)],
        [near, near_y, near_x, f_own, f_y, *turned],
        [pltpu.VMEM((cols, 2 * width), f32)],
        flops=9 * channel * width * width,
    )[0]
    inner = call(
        late_body,
        [shape((3, width, width), f32)],
        [low, high, f_x, g_own, g_y, g_x, g_d, inner, *turned],
        [pltpu.VMEM((cols, 2 * width), f32)],
        flops=9 * channel * width * width,
    )[0]
    inner_other = send(inner, to_core)
    rows = cols + block
    base, rows_high, rows_low = call(
        functools.partial(base_body, depth),
        [shape((block, cols), f32), *[shape((block, 2 * width), bf16)] * 2],
        [
            matrix, cross_high, cross_low, panel_high, panel_low, panel_rows, panel_rows_other,
            near, near_y, near_x, f_own, f_y, f_x, g_own, g_y, g_x, g_d, low, high,
            piece, piece_other, far_other,
        ],
        [
            pltpu.VMEM((channel, 2 * width), f32), pltpu.VMEM((rows, 2 * width), f32),
            pltpu.VMEM((block, 2 * width), f32),
        ],
        flops=18 * rows * width * width,
    )
    return call(
        update_body,
        [shape((block, cols), f32)],
        [
            base, inner, inner_other, cross_high, cross_low, panel_high, panel_low, rows_high,
            rows_low,
        ],
        flops=18 * rows * width * width,
    )[0]


def per_device(planes, matrix, panels, factors):
    if not planes:
        return general_device(matrix, panels, factors)
    return plane_device(matrix, panels, factors)


def solution(mesh):
    row_count, col_count = mesh.shape["row"], mesh.shape["col"]
    planes = row_count == 2 * col_count and col_count == 4
    return jax.shard_map(
        functools.partial(per_device, planes),
        mesh=mesh,
        in_specs=(P("row", "col"), P(None, ("col", "row"), None), P()),
        out_specs=P("row", "col"),
        check_vma=False,
    )
```

```python
import functools

import jax
import jax.numpy as jnp
from jax import lax
from jax.experimental import pallas as pl
from jax.experimental.pallas import tpu as pltpu
from jax.sharding import PartitionSpec as P


highest = lax.Precision.HIGHEST


def from_root(block, axis, owner):
    block = jnp.where(lax.axis_index(axis) == owner, block, jnp.zeros_like(block))
    return lax.psum(block, axis)


def matmul(left, right):
    return jnp.dot(left, right, precision=highest, preferred_element_type=jnp.float32)


def transposed_product(left, right):
    return lax.dot_general(
        left, right, (((0,), (0,)), ((), ())), precision=highest, preferred_element_type=jnp.float32
    )


def outer_product(left, right):
    return lax.dot_general(
        left, right, (((1,), (1,)), ((), ())), precision=highest, preferred_element_type=jnp.float32
    )


def general_device(matrix, panels, factors):
    row_count = lax.axis_size("row")
    col_count = lax.axis_size("col")
    my_row = lax.axis_index("row")
    block_rows = matrix.shape[0]
    share = panels.shape[1]
    source = my_row * col_count // row_count
    offset = share * (my_row * col_count - source * row_count)
    gathered = lax.all_gather(panels, "row", axis=1, tiled=True)
    relayed = from_root(gathered, "col", source)
    current = matrix
    for section in range(panels.shape[0]):
        factor = factors[section]
        panel_cols = gathered[section]
        panel_rows = lax.dynamic_slice_in_dim(relayed[section], offset, block_rows, 0)
        sums_rows = lax.psum(matmul(current, panel_cols), "col")
        sums_cols = lax.psum(transposed_product(current, panel_rows), "row")
        image_rows = matmul(sums_rows, factor)
        image_cols = matmul(sums_cols, factor)
        inner = lax.psum(transposed_product(panel_rows, image_rows), "row")
        correction = transposed_product(factor, inner)
        update_rows = image_rows - 0.5 * matmul(panel_rows, correction)
        update_cols = image_cols - 0.5 * matmul(panel_cols, correction)
        current = (
            current
            - outer_product(panel_rows, update_cols)
            - outer_product(update_rows, panel_cols)
        )
    return current


def apart3(left, right, dims=(1, 0)):
    numbers = (((dims[0],), (dims[1],)), ((), ()))
    one = functools.partial(
        lax.dot_general, dimension_numbers=numbers, preferred_element_type=jnp.float32
    )
    return one(left[0], right[0]) + (one(left[0], right[1]) + one(left[1], right[0]))


def split(value):
    high = value.astype(jnp.bfloat16)
    low = (value - high.astype(jnp.float32)).astype(jnp.bfloat16)
    return high, low


def dot3(left, right, dims=(1, 0)):
    joined_left = jnp.concatenate([left[0], left[0], left[1]], axis=dims[0])
    joined_right = jnp.concatenate([right[0], right[1], right[0]], axis=dims[1])
    numbers = (((dims[0],), (dims[1],)), ((), ()))
    return lax.dot_general(
        joined_left, joined_right, numbers, preferred_element_type=jnp.float32
    )


def place():
    row, col = lax.axis_index("row"), lax.axis_index("col")
    return row // 2, row % 2, col // 2, col % 2


def vmem(count):
    return [pl.BlockSpec(memory_space=pltpu.VMEM)] * count


def call(body, shapes, operands, scratch=(), flops=0, space=pltpu.VMEM):
    moved = sum(4 * o.size for o in operands) + sum(4 * s.size for s in shapes)
    return pl.pallas_call(
        body,
        out_shape=shapes,
        in_specs=[pl.BlockSpec(memory_space=space)] * len(operands),
        out_specs=vmem(len(shapes)),
        scratch_shapes=list(scratch),
        cost_estimate=pl.CostEstimate(flops=flops, bytes_accessed=moved, transcendentals=0),
        compiler_params=pltpu.CompilerParams(vmem_limit_bytes=20 * 1024 * 1024),
    )(*operands)


def prepare_body(matrix_hbm, panels_hbm, factors_hbm, *refs):
    high_ref, low_ref, slab_ref, factor_high, factor_low, tile, factors, sems = refs
    copies = [
        pltpu.make_async_copy(matrix_hbm, tile, sems.at[0]),
        pltpu.make_async_copy(factors_hbm, factors, sems.at[1]),
        pltpu.make_async_copy(panels_hbm, slab_ref, sems.at[2]),
    ]
    for copy in copies:
        copy.start()
    copies[0].wait()
    high_ref[...], low_ref[...] = split(tile[...])
    copies[1].wait()
    factor_high[...], factor_low[...] = split(factors[...])
    copies[2].wait()


def share_of(core, high_a, low_a, panel, factor_high, factor_low, out_ref):
    _, _, x, _ = place()
    _, _, quarter, width = out_ref.shape
    rows = [
        pl.ds(pl.multiple_of((2 * h + core) * quarter, quarter), quarter) for h in (x, 1 - x)
    ]
    tile = [jnp.concatenate([a[r, :] for r in rows], axis=0) for a in (high_a, low_a)]
    product = dot3(tile, panel)
    for step in range(2):
        factor = (factor_high[step], factor_low[step])
        image = dot3(split(product[:, step * width : (step + 1) * width]), factor)
        for side in range(2):
            out_ref[side, step] = image[side * quarter : (side + 1) * quarter]


def give_body(depth, high_a, low_a, factor_high, factor_low, *refs):
    slabs, (give_ref, high, low) = refs[: 2 * depth], refs[2 * depth :]
    z, y, _, k = place()
    share, width = slabs[0].shape[1], slabs[0].shape[2]
    for flip in range(2):
        for shift in range(depth):
            slab = slabs[flip * depth + shift]
            at = 2 * lax.rem(z - shift + depth, depth) + (1 - y if flip else y)
            rows = pl.ds(pl.multiple_of(at * share, share), share)
            for step in range(2):
                h, l = split(slab[step])
                high[rows, step * width : (step + 1) * width] = h
                low[rows, step * width : (step + 1) * width] = l
    panel = (high[...], low[...])
    share_of(1 - k, high_a, low_a, panel, factor_high, factor_low, give_ref)


def keep_body(high_a, low_a, factor_high, factor_low, high, low, keep_ref):
    _, _, _, k = place()
    share_of(k, high_a, low_a, (high[...], low[...]), factor_high, factor_low, keep_ref)


EARLY = (("a", 0), ("b", 0), ("a", 1), ("b", 1), ("a", 2), ("b", 2), ("f", 0), ("f", 1))
LATE = (("a", 3), ("b", 3), ("f", 2), ("f", 3), ("g", 0), ("g", 1), ("g", 2), ("g", 3))


def row_of(depth, kind, flip, quarter):
    z, y, x, k = place()
    owner = z % 2 == k
    if kind in "ab":
        plane = jnp.where(owner, z, z + 1 - 2 * (z % 2))
    else:
        plane = jnp.where(owner, lax.rem(z + 2, depth), depth - 1 - z)
    inner = jnp.where((z == 0) | (z == depth - 1), k, 1 - k)
    core = {"a": k, "b": 1 - k, "f": inner, "g": 1 - inner}[kind]
    y_from = 1 - y if flip & 1 else y
    x_from = 1 - x if flip & 2 else x
    block = (plane // 2) * 4 + y_from * 2 + x_from
    return pl.multiple_of((2 * block + core) * quarter, quarter)


def fill(image, start, parts):
    for step, part in enumerate(parts):
        quarter, width = part.shape
        image[pl.ds(start, quarter), step * width : (step + 1) * width] = part[...]


def steps(ref):
    return ref.at[0], ref.at[1]


def near_pieces(flip, ref):
    return {("a", flip): steps(ref.at[0]), ("b", flip): steps(ref.at[1])}


def corner_pieces(low, high):
    return {
        ("a", 3): (low.at[0], low.at[1]),
        ("b", 3): (high.at[0], high.at[1]),
        ("f", 3): (low.at[2], high.at[2]),
    }


def panel_body(depth, *refs):
    factor_high, factor_low, across_ref, opposite_ref = refs[:4]
    slabs = refs[4 : 4 + 2 * depth]
    (
        turn1_high, turn1_low, turn2_ref, turn3_high, turn3_low, cross_ref, rows_ref,
         full, turning,
    ) = refs[4 + 2 * depth :]
    z, y, x, _ = place()
    share, width = slabs[0].shape[1], slabs[0].shape[2]
    column = 2 * depth * share
    for across in range(2):
        for flip in range(2):
            for shift in range(depth):
                if across:
                    slab = (opposite_ref if flip else across_ref).at[shift]
                else:
                    slab = slabs[flip * depth + shift]
                at = 2 * lax.rem(z - shift + depth, depth) + (1 - y if flip else y)
                start = (1 - x if across else x) * column + at * share
                fill(full, pl.multiple_of(start, share), steps(slab))
    for at, (kind, flip) in enumerate(EARLY + LATE):
        rows = pl.ds(row_of(depth, kind, flip, share), share)
        turning[at * share : (at + 1) * share, :] = full[rows, :]
    first, second = split(turning[:, :width]), split(turning[:, width:])
    turn1_high[...], turn1_low[...] = split(
        0.5 * dot3((factor_high[0], factor_low[0]), first, (0, 1))
    )
    turn2 = dot3((factor_high[1], factor_low[1]), second, (0, 1))
    turn2_ref[...] = turn2
    turn3_high[...], turn3_low[...] = split(0.5 * turn2)
    cross_ref[...] = dot3(first, second, (0, 0))
    block = 4 * share
    start = (z // 2) * column + y * block
    rows_ref[...] = full[pl.ds(pl.multiple_of(start, block), block), :]


def cross_body(
    factor_high, factor_low, cross_a, cross_b, turn1_high, turn1_low, turn2_ref,
    mixed_high, mixed_low, out_high, out_low,
):
    cross = split(dot3(split(cross_a[...] + cross_b[...]), (factor_high[1], factor_low[1])))
    mixed_high[...], mixed_low[...] = cross
    turned = turn2_ref[...] - dot3(cross, (turn1_high[...], turn1_low[...]), (0, 0))
    out_high[...], out_low[...] = split(turned)


def products(turned, image, span):
    width = image.shape[1] // 2
    high, low = split(image[...])
    for (turn_high, turn_low), p in zip(turned, (0, 0, width)):
        side = slice(p, p + width)
        yield dot3((turn_high[:, span], turn_low[:, span]), (high[:, side], low[:, side]))


def early_body(near, near_y, near_x, f_own, f_y, *refs):
    turned, (inner_ref, image) = refs[:6], refs[6:]
    held = {("f", 0): steps(f_own), ("f", 1): steps(f_y)}
    for flip, ref in enumerate((near, near_y, near_x)):
        held.update(near_pieces(flip, ref))
    quarter = near.shape[2]
    for at, key in enumerate(EARLY):
        fill(image, at * quarter, held[key])
    pairs = (turned[0:2], turned[2:4], turned[4:6])
    for at, value in enumerate(products(pairs, image, slice(0, image.shape[0]))):
        inner_ref[at] = value


def late_body(low, high, f_x, g_own, g_y, g_x, g_d, before, *refs):
    turned, (inner_ref, image) = refs[:6], refs[6:]
    held = {("f", 2): steps(f_x), **corner_pieces(low, high)}
    for flip, ref in enumerate((g_own, g_y, g_x, g_d)):
        held["g", flip] = steps(ref)
    quarter = low.shape[1]
    for at, key in enumerate(LATE):
        fill(image, at * quarter, held[key])
    pairs = (turned[0:2], turned[2:4], turned[4:6])
    span = slice(image.shape[0], 2 * image.shape[0])
    for at, value in enumerate(products(pairs, image, span)):
        inner_ref[at] = before[at] + value


def base_body(depth, *refs):
    (
        matrix_ref, cross_high, cross_low, high_ref, low_ref, panel_a, panel_b,
        near, near_y, near_x, f_own, f_y, f_x, g_own, g_y, g_x, g_d, low, high,
        piece_a, piece_b, far_b, out_ref, rows_high, rows_low, full, image, rows_v,
    ) = refs
    z, _, x, k = place()
    owner = z % 2 == k
    quarter, width = low.shape[1], low.shape[2]
    cols = high_ref.shape[0]
    held = {("f", 0): steps(f_own), ("f", 1): steps(f_y), ("f", 2): steps(f_x)}
    held.update(corner_pieces(low, high))
    for flip, ref in enumerate((near, near_y, near_x)):
        held.update(near_pieces(flip, ref))
    for flip, ref in enumerate((g_own, g_y, g_x, g_d)):
        held["g", flip] = steps(ref)
    for (kind, flip), parts in held.items():
        fill(full, row_of(depth, kind, flip, quarter), parts)
    image[pl.ds(0, cols), :] = full[pl.ds(pl.multiple_of(x * cols, cols), cols), :]

    def row(side, core):
        return pl.multiple_of(cols + (2 * side + core) * quarter, quarter)

    fill(image, row(x, k), steps(piece_a))
    fill(image, row(x, 1 - k), steps(piece_b))

    @pl.when(owner)
    def _():
        for at, core in enumerate((k, 1 - k)):
            fill(image, row(1 - x, core), steps(near_x.at[at]))
        rows_v[...] = panel_a[...]

    @pl.when(jnp.logical_not(owner))
    def _():
        for at, core in enumerate((1 - k, k)):
            fill(image, row(1 - x, core), steps(far_b.at[at]))
        rows_v[...] = panel_b[...]

    first, second = slice(0, width), slice(width, 2 * width)
    w1 = split(image[:, first])
    w2 = split(image[:, second] - dot3(w1, (cross_high[...], cross_low[...])))
    v_rows = split(rows_v[...])
    rows_high[...], rows_low[...] = v_rows
    total = matrix_ref[...]
    for w, at in ((w1, first), (w2, second)):
        v_side = (high_ref[:, at], low_ref[:, at])
        v_top = [v[:, at] for v in v_rows]
        total = total - dot3(v_top, [p[:cols] for p in w], (1, 1))
        total = total - dot3([p[cols:] for p in w], v_side, (1, 1))
    out_ref[...] = total


def update_body(
    base_ref, inner_a, inner_b, cross_high, cross_low, high_ref, low_ref, rows_high, rows_low,
    out_ref,
):
    width = cross_high.shape[0]
    first, second = slice(0, width), slice(width, 2 * width)
    cross = (cross_high[...], cross_low[...])
    v1 = (rows_high[:, first], rows_low[:, first])
    v2 = (rows_high[:, second], rows_low[:, second])
    m1 = inner_a[0] + inner_b[0]
    mixed_t = inner_a[1] + inner_b[1]
    m2 = inner_a[2] + inner_b[2]
    taken = split(apart3(split(mixed_t), cross))
    side = split(mixed_t.T - apart3(split(m1), cross))
    left = apart3(v1, split(m1 + m1.T)) + apart3(v2, side, (1, 1))
    right = apart3(v2, split(m2 + m2.T)) - apart3(v2, taken) - apart3(v2, taken, (1, 1))
    right = right + apart3(v1, side)
    out_ref[...] = (
        base_ref[...]
        + apart3(split(left), (high_ref[:, first], low_ref[:, first]), (1, 1))
        + apart3(split(right), (high_ref[:, second], low_ref[:, second]), (1, 1))
    )


def plane_device(matrix, panels, factors):
    row_count, col_count = lax.axis_size("row"), lax.axis_size("col")
    depth = row_count // 2
    z, _, _, k = place()
    owner = z % 2 == k
    f32, bf16 = jnp.float32, jnp.bfloat16
    shape = jax.ShapeDtypeStruct

    def send(value, target):
        pairs = []
        for index in range(row_count * col_count):
            row, col = divmod(index, col_count)
            to = target(row // 2, row % 2, col // 2, col % 2)
            pairs.append((index, (to[0] * 2 + to[1]) * col_count + to[2] * 2 + to[3]))
        return lax.ppermute(value, ("row", "col"), pairs)

    def along_z(shift):
        return lambda z, y, x, k: ((z + shift) % depth, y, x, k)

    def to_y(z, y, x, k):
        return z, 1 - y, x, k

    def to_x(z, y, x, k):
        return z, y, 1 - x, k

    def to_corner(z, y, x, k):
        return z, 1 - y, 1 - x, k

    def to_core(z, y, x, k):
        return z, y, x, 1 - k

    def ahead(first):
        def target(z, y, x, k):
            outer = z in (0, depth - 1)
            far = ((k == z % 2) == first) == outer
            return (depth - 1 - z if far else (z + 2) % depth), y, x, z % 2

        return target

    def back_first(z, y, x, k):
        return z ^ 1 if k == z % 2 else z, y, x, z % 2

    def back_second(z, y, x, k):
        return (z, y, 1 - x, k) if k == z % 2 else (z ^ 1, y, x, z % 2)

    _, _, width = panels.shape
    block, cols = matrix.shape
    quarter, channel = block // 4, 2 * cols

    high_a, low_a, slab, factor_high, factor_low = call(
        prepare_body,
        [
            shape(matrix.shape, bf16), shape(matrix.shape, bf16), shape(panels.shape, f32),
            shape(factors.shape, bf16), shape(factors.shape, bf16),
        ],
        [matrix, panels, factors],
        [
            pltpu.VMEM(matrix.shape, f32), pltpu.VMEM(factors.shape, f32),
            pltpu.SemaphoreType.DMA((3,)),
        ],
        space=pltpu.HBM,
    )

    order = [2, 1] + list(range(3, depth))
    slabs = {0: slab}
    for shift in order:
        slabs[shift] = send(panels, along_z(shift))
    own = [slabs[s] for s in range(depth)]
    beside = [send(slabs[s], to_y) for s in range(depth)]
    across = [send(slabs[s], to_x) for s in range(depth)]

    share_shape, cols_shape = shape((2, 2, quarter, width), f32), shape((cols, 2 * width), bf16)
    held = [high_a, low_a, factor_high, factor_low]
    give, panel_high, panel_low = call(
        functools.partial(give_body, depth),
        [share_shape, cols_shape, cols_shape],
        [*held, *own, *beside],
        flops=3 * block * cols * width * 2,
    )
    keep = call(
        keep_body, [share_shape], [*held, panel_high, panel_low], flops=3 * block * cols * width * 2
    )[0]
    chip = keep + send(give, to_core)
    piece = chip[0] + send(chip[1], to_x)

    stacked = jnp.stack(across)
    opposite = send(stacked, to_y)
    turn1_high, turn1_low, turn2, turn3_high, turn3_low, cross, panel_rows = call(
        functools.partial(panel_body, depth),
        [
            *[shape((width, channel), bf16)] * 2,
            shape((width, channel), f32),
            *[shape((width, channel), bf16)] * 2,
            shape((width, width), f32),
            shape((block, 2 * width), f32),
        ],
        [factor_high, factor_low, stacked, opposite, *own, *beside],
        [pltpu.VMEM((channel, 2 * width), f32)] * 2,
        flops=6 * channel * width * width * 3,
    )
    cross_other = send(cross, to_core)
    cross_high, cross_low, turn2_high, turn2_low = call(
        cross_body,
        [*[shape((width, width), bf16)] * 2, *[shape((width, channel), bf16)] * 2],
        [factor_high, factor_low, cross, cross_other, turn1_high, turn1_low, turn2],
        flops=6 * channel * width * width,
    )
    turned = [turn1_high, turn1_low, turn2_high, turn2_low, turn3_high, turn3_low]
    panel_rows_other = send(panel_rows, to_core)

    back1, back2 = send(piece, back_first), send(piece, back_second)
    f_own, g_own = send(piece, ahead(True)), send(piece, ahead(False))
    near = jnp.where(owner, jnp.stack([piece, back1]), jnp.stack([back1, back2]))
    near_y, near_x = send(near, to_y), send(near, to_x)
    f_y, f_x = send(f_own, to_y), send(f_own, to_x)
    g_y, g_x = send(g_own, to_y), send(g_own, to_x)
    g_d = send(g_own, to_corner)
    low = jnp.concatenate([near_x[0], f_x[:1]])
    high = jnp.concatenate([near_y[1], f_y[1:]])
    low, high = send(low, to_y), send(high, to_x)
    piece_other = send(piece, to_core)
    far_other = send(near_x, to_core)

    inner = call(
        early_body,
        [shape((3, width, width), f32)],
        [near, near_y, near_x, f_own, f_y, *turned],
        [pltpu.VMEM((cols, 2 * width), f32)],
        flops=9 * channel * width * width,
    )[0]
    inner = call(
        late_body,
        [shape((3, width, width), f32)],
        [low, high, f_x, g_own, g_y, g_x, g_d, inner, *turned],
        [pltpu.VMEM((cols, 2 * width), f32)],
        flops=9 * channel * width * width,
    )[0]
    inner_other = send(inner, to_core)
    rows = cols + block
    base, rows_high, rows_low = call(
        functools.partial(base_body, depth),
        [shape((block, cols), f32), *[shape((block, 2 * width), bf16)] * 2],
        [
            matrix, cross_high, cross_low, panel_high, panel_low, panel_rows, panel_rows_other,
            near, near_y, near_x, f_own, f_y, f_x, g_own, g_y, g_x, g_d, low, high,
            piece, piece_other, far_other,
        ],
        [
            pltpu.VMEM((channel, 2 * width), f32), pltpu.VMEM((rows, 2 * width), f32),
            pltpu.VMEM((block, 2 * width), f32),
        ],
        flops=18 * rows * width * width,
    )
    return call(
        update_body,
        [shape((block, cols), f32)],
        [
            base, inner, inner_other, cross_high, cross_low, panel_high, panel_low, rows_high,
            rows_low,
        ],
        flops=18 * rows * width * width,
    )[0]


def per_device(planes, matrix, panels, factors):
    if not planes:
        return general_device(matrix, panels, factors)
    return plane_device(matrix, panels, factors)


def solution(mesh):
    row_count, col_count = mesh.shape["row"], mesh.shape["col"]
    planes = row_count == 2 * col_count and col_count == 4
    return jax.shard_map(
        functools.partial(per_device, planes),
        mesh=mesh,
        in_specs=(P("row", "col"), P(None, ("col", "row"), None), P()),
        out_specs=P("row", "col"),
        check_vma=False,
    )
```

```python
import functools

import jax
import jax.numpy as jnp
from jax import lax
from jax.experimental import pallas as pl
from jax.experimental.pallas import tpu as pltpu
from jax.sharding import PartitionSpec as P


highest = lax.Precision.HIGHEST


def from_root(block, axis, owner):
    block = jnp.where(lax.axis_index(axis) == owner, block, jnp.zeros_like(block))
    return lax.psum(block, axis)


def matmul(left, right):
    return jnp.dot(left, right, precision=highest, preferred_element_type=jnp.float32)


def transposed_product(left, right):
    return lax.dot_general(
        left, right, (((0,), (0,)), ((), ())), precision=highest, preferred_element_type=jnp.float32
    )


def outer_product(left, right):
    return lax.dot_general(
        left, right, (((1,), (1,)), ((), ())), precision=highest, preferred_element_type=jnp.float32
    )


def general_device(matrix, panels, factors):
    row_count = lax.axis_size("row")
    col_count = lax.axis_size("col")
    my_row = lax.axis_index("row")
    block_rows = matrix.shape[0]
    share = panels.shape[1]
    source = my_row * col_count // row_count
    offset = share * (my_row * col_count - source * row_count)
    gathered = lax.all_gather(panels, "row", axis=1, tiled=True)
    relayed = from_root(gathered, "col", source)
    current = matrix
    for section in range(panels.shape[0]):
        factor = factors[section]
        panel_cols = gathered[section]
        panel_rows = lax.dynamic_slice_in_dim(relayed[section], offset, block_rows, 0)
        sums_rows = lax.psum(matmul(current, panel_cols), "col")
        sums_cols = lax.psum(transposed_product(current, panel_rows), "row")
        image_rows = matmul(sums_rows, factor)
        image_cols = matmul(sums_cols, factor)
        inner = lax.psum(transposed_product(panel_rows, image_rows), "row")
        correction = transposed_product(factor, inner)
        update_rows = image_rows - 0.5 * matmul(panel_rows, correction)
        update_cols = image_cols - 0.5 * matmul(panel_cols, correction)
        current = (
            current
            - outer_product(panel_rows, update_cols)
            - outer_product(update_rows, panel_cols)
        )
    return current


def apart3(left, right, dims=(1, 0)):
    numbers = (((dims[0],), (dims[1],)), ((), ()))
    one = functools.partial(
        lax.dot_general, dimension_numbers=numbers, preferred_element_type=jnp.float32
    )
    return one(left[0], right[0]) + (one(left[0], right[1]) + one(left[1], right[0]))


def split(value):
    high = value.astype(jnp.bfloat16)
    low = (value - high.astype(jnp.float32)).astype(jnp.bfloat16)
    return high, low


def dot3(left, right, dims=(1, 0)):
    joined_left = jnp.concatenate([left[0], left[0], left[1]], axis=dims[0])
    joined_right = jnp.concatenate([right[0], right[1], right[0]], axis=dims[1])
    numbers = (((dims[0],), (dims[1],)), ((), ()))
    return lax.dot_general(
        joined_left, joined_right, numbers, preferred_element_type=jnp.float32
    )


def place():
    row, col = lax.axis_index("row"), lax.axis_index("col")
    return row // 2, row % 2, col // 2, col % 2


def vmem(count):
    return [pl.BlockSpec(memory_space=pltpu.VMEM)] * count


def call(body, shapes, operands, scratch=(), flops=0, space=pltpu.VMEM):
    moved = sum(4 * o.size for o in operands) + sum(4 * s.size for s in shapes)
    return pl.pallas_call(
        body,
        out_shape=shapes,
        in_specs=[pl.BlockSpec(memory_space=space)] * len(operands),
        out_specs=vmem(len(shapes)),
        scratch_shapes=list(scratch),
        cost_estimate=pl.CostEstimate(flops=flops, bytes_accessed=moved, transcendentals=0),
        compiler_params=pltpu.CompilerParams(vmem_limit_bytes=20 * 1024 * 1024),
    )(*operands)


def prepare_body(matrix_hbm, panels_hbm, factors_hbm, *refs):
    high_ref, low_ref, slab_ref, factor_high, factor_low, tile, factors, sems = refs
    copies = [
        pltpu.make_async_copy(matrix_hbm, tile, sems.at[0]),
        pltpu.make_async_copy(factors_hbm, factors, sems.at[1]),
        pltpu.make_async_copy(panels_hbm, slab_ref, sems.at[2]),
    ]
    for copy in copies:
        copy.start()
    copies[0].wait()
    high_ref[...], low_ref[...] = split(tile[...])
    copies[1].wait()
    factor_high[...], factor_low[...] = split(factors[...])
    copies[2].wait()


def share_of(core, high_a, low_a, panel, factor_high, factor_low, out_ref):
    _, _, x, _ = place()
    _, _, quarter, width = out_ref.shape
    rows = [
        pl.ds(pl.multiple_of((2 * h + core) * quarter, quarter), quarter) for h in (x, 1 - x)
    ]
    tile = [jnp.concatenate([a[r, :] for r in rows], axis=0) for a in (high_a, low_a)]
    product = dot3(tile, panel)
    for step in range(2):
        factor = (factor_high[step], factor_low[step])
        image = dot3(split(product[:, step * width : (step + 1) * width]), factor)
        for side in range(2):
            out_ref[side, step] = image[side * quarter : (side + 1) * quarter]


def give_body(depth, high_a, low_a, factor_high, factor_low, *refs):
    slabs, (give_ref, high, low) = refs[: 2 * depth], refs[2 * depth :]
    z, y, _, k = place()
    share, width = slabs[0].shape[1], slabs[0].shape[2]
    for flip in range(2):
        for shift in range(depth):
            slab = slabs[flip * depth + shift]
            at = 2 * (z ^ shift) + (1 - y if flip else y)
            rows = pl.ds(pl.multiple_of(at * share, share), share)
            for step in range(2):
                h, l = split(slab[step])
                high[rows, step * width : (step + 1) * width] = h
                low[rows, step * width : (step + 1) * width] = l
    panel = (high[...], low[...])
    share_of(1 - k, high_a, low_a, panel, factor_high, factor_low, give_ref)


def keep_body(high_a, low_a, factor_high, factor_low, high, low, keep_ref):
    _, _, _, k = place()
    share_of(k, high_a, low_a, (high[...], low[...]), factor_high, factor_low, keep_ref)


EARLY = (("a", 0), ("b", 0), ("a", 1), ("b", 1), ("a", 2), ("b", 2), ("f", 0), ("f", 1))
LATE = (("a", 3), ("b", 3), ("f", 2), ("f", 3), ("g", 0), ("g", 1), ("g", 2), ("g", 3))


def row_of(depth, kind, flip, quarter):
    z, y, x, k = place()
    owner = z % 2 == k
    if kind in "ab":
        plane = jnp.where(owner, z, z + 1 - 2 * (z % 2))
    else:
        plane = jnp.where(owner, lax.rem(z + 2, depth), depth - 1 - z)
    inner = jnp.where((z == 0) | (z == depth - 1), k, 1 - k)
    core = {"a": k, "b": 1 - k, "f": inner, "g": 1 - inner}[kind]
    y_from = 1 - y if flip & 1 else y
    x_from = 1 - x if flip & 2 else x
    block = (plane // 2) * 4 + y_from * 2 + x_from
    return pl.multiple_of((2 * block + core) * quarter, quarter)


def fill(image, start, parts):
    for step, part in enumerate(parts):
        quarter, width = part.shape
        image[pl.ds(start, quarter), step * width : (step + 1) * width] = part[...]


def steps(ref):
    return ref.at[0], ref.at[1]


def near_pieces(flip, ref):
    return {("a", flip): steps(ref.at[0]), ("b", flip): steps(ref.at[1])}


def corner_pieces(low, high):
    return {
        ("a", 3): (low.at[0], low.at[1]),
        ("b", 3): (high.at[0], high.at[1]),
        ("f", 3): (low.at[2], high.at[2]),
    }


def panel_body(depth, *refs):
    factor_high, factor_low, across_ref, opposite_ref = refs[:4]
    slabs = refs[4 : 4 + 2 * depth]
    (
        turn1_high, turn1_low, turn2_ref, turn3_high, turn3_low, cross_ref, rows_ref,
         full, turning,
    ) = refs[4 + 2 * depth :]
    z, y, x, _ = place()
    share, width = slabs[0].shape[1], slabs[0].shape[2]
    column = 2 * depth * share
    for across in range(2):
        for flip in range(2):
            for shift in range(depth):
                if across:
                    slab = (opposite_ref if flip else across_ref).at[shift]
                else:
                    slab = slabs[flip * depth + shift]
                at = 2 * (z ^ shift) + (1 - y if flip else y)
                start = (1 - x if across else x) * column + at * share
                fill(full, pl.multiple_of(start, share), steps(slab))
    for at, (kind, flip) in enumerate(EARLY + LATE):
        rows = pl.ds(row_of(depth, kind, flip, share), share)
        turning[at * share : (at + 1) * share, :] = full[rows, :]
    first, second = split(turning[:, :width]), split(turning[:, width:])
    turn1_high[...], turn1_low[...] = split(
        0.5 * dot3((factor_high[0], factor_low[0]), first, (0, 1))
    )
    turn2 = dot3((factor_high[1], factor_low[1]), second, (0, 1))
    turn2_ref[...] = turn2
    turn3_high[...], turn3_low[...] = split(0.5 * turn2)
    cross_ref[...] = dot3(first, second, (0, 0))
    block = 4 * share
    start = (z // 2) * column + y * block
    rows_ref[...] = full[pl.ds(pl.multiple_of(start, block), block), :]


def cross_body(
    factor_high, factor_low, cross_a, cross_b, turn1_high, turn1_low, turn2_ref,
    mixed_high, mixed_low, out_high, out_low,
):
    cross = split(dot3(split(cross_a[...] + cross_b[...]), (factor_high[1], factor_low[1])))
    mixed_high[...], mixed_low[...] = cross
    turned = turn2_ref[...] - dot3(cross, (turn1_high[...], turn1_low[...]), (0, 0))
    out_high[...], out_low[...] = split(turned)


def products(turned, image, span):
    width = image.shape[1] // 2
    high, low = split(image[...])
    for (turn_high, turn_low), p in zip(turned, (0, 0, width)):
        side = slice(p, p + width)
        yield dot3((turn_high[:, span], turn_low[:, span]), (high[:, side], low[:, side]))


def early_body(near, near_y, near_x, f_own, f_y, *refs):
    turned, (inner_ref, image) = refs[:6], refs[6:]
    held = {("f", 0): steps(f_own), ("f", 1): steps(f_y)}
    for flip, ref in enumerate((near, near_y, near_x)):
        held.update(near_pieces(flip, ref))
    quarter = near.shape[2]
    for at, key in enumerate(EARLY):
        fill(image, at * quarter, held[key])
    pairs = (turned[0:2], turned[2:4], turned[4:6])
    for at, value in enumerate(products(pairs, image, slice(0, image.shape[0]))):
        inner_ref[at] = value


def late_body(low, high, f_x, g_own, g_y, g_x, g_d, before, *refs):
    turned, (inner_ref, image) = refs[:6], refs[6:]
    held = {("f", 2): steps(f_x), **corner_pieces(low, high)}
    for flip, ref in enumerate((g_own, g_y, g_x, g_d)):
        held["g", flip] = steps(ref)
    quarter = low.shape[1]
    for at, key in enumerate(LATE):
        fill(image, at * quarter, held[key])
    pairs = (turned[0:2], turned[2:4], turned[4:6])
    span = slice(image.shape[0], 2 * image.shape[0])
    for at, value in enumerate(products(pairs, image, span)):
        inner_ref[at] = before[at] + value


def base_body(depth, *refs):
    (
        matrix_ref, cross_high, cross_low, high_ref, low_ref, panel_a, panel_b,
        near, near_y, near_x, f_own, f_y, f_x, g_own, g_y, g_x, g_d, low, high,
        piece_a, piece_b, far_b, out_ref, rows_high, rows_low, full, image, rows_v,
    ) = refs
    z, _, x, k = place()
    owner = z % 2 == k
    quarter, width = low.shape[1], low.shape[2]
    cols = high_ref.shape[0]
    held = {("f", 0): steps(f_own), ("f", 1): steps(f_y), ("f", 2): steps(f_x)}
    held.update(corner_pieces(low, high))
    for flip, ref in enumerate((near, near_y, near_x)):
        held.update(near_pieces(flip, ref))
    for flip, ref in enumerate((g_own, g_y, g_x, g_d)):
        held["g", flip] = steps(ref)
    for (kind, flip), parts in held.items():
        fill(full, row_of(depth, kind, flip, quarter), parts)
    image[pl.ds(0, cols), :] = full[pl.ds(pl.multiple_of(x * cols, cols), cols), :]

    def row(side, core):
        return pl.multiple_of(cols + (2 * side + core) * quarter, quarter)

    fill(image, row(x, k), steps(piece_a))
    fill(image, row(x, 1 - k), steps(piece_b))

    @pl.when(owner)
    def _():
        for at, core in enumerate((k, 1 - k)):
            fill(image, row(1 - x, core), steps(near_x.at[at]))
        rows_v[...] = panel_a[...]

    @pl.when(jnp.logical_not(owner))
    def _():
        for at, core in enumerate((1 - k, k)):
            fill(image, row(1 - x, core), steps(far_b.at[at]))
        rows_v[...] = panel_b[...]

    first, second = slice(0, width), slice(width, 2 * width)
    w1 = split(image[:, first])
    w2 = split(image[:, second] - dot3(w1, (cross_high[...], cross_low[...])))
    v_rows = split(rows_v[...])
    rows_high[...], rows_low[...] = v_rows
    total = matrix_ref[...]
    for w, at in ((w1, first), (w2, second)):
        v_side = (high_ref[:, at], low_ref[:, at])
        v_top = [v[:, at] for v in v_rows]
        total = total - dot3(v_top, [p[:cols] for p in w], (1, 1))
        total = total - dot3([p[cols:] for p in w], v_side, (1, 1))
    out_ref[...] = total


def update_body(
    base_ref, inner_a, inner_b, cross_high, cross_low, high_ref, low_ref, rows_high, rows_low,
    out_ref,
):
    width = cross_high.shape[0]
    first, second = slice(0, width), slice(width, 2 * width)
    cross = (cross_high[...], cross_low[...])
    v1 = (rows_high[:, first], rows_low[:, first])
    v2 = (rows_high[:, second], rows_low[:, second])
    m1 = inner_a[0] + inner_b[0]
    mixed_t = inner_a[1] + inner_b[1]
    m2 = inner_a[2] + inner_b[2]
    taken = split(apart3(split(mixed_t), cross))
    side = split(mixed_t.T - apart3(split(m1), cross))
    left = apart3(v1, split(m1 + m1.T)) + apart3(v2, side, (1, 1))
    right = apart3(v2, split(m2 + m2.T)) - apart3(v2, taken) - apart3(v2, taken, (1, 1))
    right = right + apart3(v1, side)
    out_ref[...] = (
        base_ref[...]
        + apart3(split(left), (high_ref[:, first], low_ref[:, first]), (1, 1))
        + apart3(split(right), (high_ref[:, second], low_ref[:, second]), (1, 1))
    )


def plane_device(matrix, panels, factors):
    row_count, col_count = lax.axis_size("row"), lax.axis_size("col")
    depth = row_count // 2
    z, _, _, k = place()
    owner = z % 2 == k
    f32, bf16 = jnp.float32, jnp.bfloat16
    shape = jax.ShapeDtypeStruct

    def send(value, target):
        pairs = []
        for index in range(row_count * col_count):
            row, col = divmod(index, col_count)
            to = target(row // 2, row % 2, col // 2, col % 2)
            pairs.append((index, (to[0] * 2 + to[1]) * col_count + to[2] * 2 + to[3]))
        return lax.ppermute(value, ("row", "col"), pairs)

    def along_z(shift):
        return lambda z, y, x, k: (z ^ shift, y, x, k)

    def to_y(z, y, x, k):
        return z, 1 - y, x, k

    def to_x(z, y, x, k):
        return z, y, 1 - x, k

    def to_corner(z, y, x, k):
        return z, 1 - y, 1 - x, k

    def to_core(z, y, x, k):
        return z, y, x, 1 - k

    def ahead(first):
        def target(z, y, x, k):
            outer = z in (0, depth - 1)
            far = ((k == z % 2) == first) == outer
            return (depth - 1 - z if far else (z + 2) % depth), y, x, z % 2

        return target

    def back_first(z, y, x, k):
        return z ^ 1 if k == z % 2 else z, y, x, z % 2

    def back_second(z, y, x, k):
        return (z, y, 1 - x, k) if k == z % 2 else (z ^ 1, y, x, z % 2)

    _, _, width = panels.shape
    block, cols = matrix.shape
    quarter, channel = block // 4, 2 * cols

    high_a, low_a, slab, factor_high, factor_low = call(
        prepare_body,
        [
            shape(matrix.shape, bf16), shape(matrix.shape, bf16), shape(panels.shape, f32),
            shape(factors.shape, bf16), shape(factors.shape, bf16),
        ],
        [matrix, panels, factors],
        [
            pltpu.VMEM(matrix.shape, f32), pltpu.VMEM(factors.shape, f32),
            pltpu.SemaphoreType.DMA((3,)),
        ],
        space=pltpu.HBM,
    )

    order = [2, 1] + list(range(3, depth))
    slabs = {0: slab}
    for shift in order:
        slabs[shift] = send(panels, along_z(shift))
    own = [slabs[s] for s in range(depth)]
    beside = [send(slabs[s], to_y) for s in range(depth)]
    across = [send(slabs[s], to_x) for s in range(depth)]

    share_shape, cols_shape = shape((2, 2, quarter, width), f32), shape((cols, 2 * width), bf16)
    held = [high_a, low_a, factor_high, factor_low]
    give, panel_high, panel_low = call(
        functools.partial(give_body, depth),
        [share_shape, cols_shape, cols_shape],
        [*held, *own, *beside],
        flops=3 * block * cols * width * 2,
    )
    keep = call(
        keep_body, [share_shape], [*held, panel_high, panel_low], flops=3 * block * cols * width * 2
    )[0]
    chip = keep + send(give, to_core)
    piece = chip[0] + send(chip[1], to_x)

    stacked = jnp.stack(across)
    opposite = send(stacked, to_y)
    turn1_high, turn1_low, turn2, turn3_high, turn3_low, cross, panel_rows = call(
        functools.partial(panel_body, depth),
        [
            *[shape((width, channel), bf16)] * 2,
            shape((width, channel), f32),
            *[shape((width, channel), bf16)] * 2,
            shape((width, width), f32),
            shape((block, 2 * width), f32),
        ],
        [factor_high, factor_low, stacked, opposite, *own, *beside],
        [pltpu.VMEM((channel, 2 * width), f32)] * 2,
        flops=6 * channel * width * width * 3,
    )
    cross_other = send(cross, to_core)
    cross_high, cross_low, turn2_high, turn2_low = call(
        cross_body,
        [*[shape((width, width), bf16)] * 2, *[shape((width, channel), bf16)] * 2],
        [factor_high, factor_low, cross, cross_other, turn1_high, turn1_low, turn2],
        flops=6 * channel * width * width,
    )
    turned = [turn1_high, turn1_low, turn2_high, turn2_low, turn3_high, turn3_low]
    panel_rows_other = send(panel_rows, to_core)

    back1, back2 = send(piece, back_first), send(piece, back_second)
    f_own, g_own = send(piece, ahead(True)), send(piece, ahead(False))
    near = jnp.where(owner, jnp.stack([piece, back1]), jnp.stack([back1, back2]))
    near_y, near_x = send(near, to_y), send(near, to_x)
    f_y, f_x = send(f_own, to_y), send(f_own, to_x)
    g_y, g_x = send(g_own, to_y), send(g_own, to_x)
    g_d = send(g_own, to_corner)
    low = jnp.concatenate([near_x[0], f_x[:1]])
    high = jnp.concatenate([near_y[1], f_y[1:]])
    low, high = send(low, to_y), send(high, to_x)
    piece_other = send(piece, to_core)
    far_other = send(near_x, to_core)

    inner = call(
        early_body,
        [shape((3, width, width), f32)],
        [near, near_y, near_x, f_own, f_y, *turned],
        [pltpu.VMEM((cols, 2 * width), f32)],
        flops=9 * channel * width * width,
    )[0]
    inner = call(
        late_body,
        [shape((3, width, width), f32)],
        [low, high, f_x, g_own, g_y, g_x, g_d, inner, *turned],
        [pltpu.VMEM((cols, 2 * width), f32)],
        flops=9 * channel * width * width,
    )[0]
    inner_other = send(inner, to_core)
    rows = cols + block
    base, rows_high, rows_low = call(
        functools.partial(base_body, depth),
        [shape((block, cols), f32), *[shape((block, 2 * width), bf16)] * 2],
        [
            matrix, cross_high, cross_low, panel_high, panel_low, panel_rows, panel_rows_other,
            near, near_y, near_x, f_own, f_y, f_x, g_own, g_y, g_x, g_d, low, high,
            piece, piece_other, far_other,
        ],
        [
            pltpu.VMEM((channel, 2 * width), f32), pltpu.VMEM((rows, 2 * width), f32),
            pltpu.VMEM((block, 2 * width), f32),
        ],
        flops=18 * rows * width * width,
    )
    return call(
        update_body,
        [shape((block, cols), f32)],
        [
            base, inner, inner_other, cross_high, cross_low, panel_high, panel_low, rows_high,
            rows_low,
        ],
        flops=18 * rows * width * width,
    )[0]


def per_device(planes, matrix, panels, factors):
    if not planes:
        return general_device(matrix, panels, factors)
    return plane_device(matrix, panels, factors)


def solution(mesh):
    row_count, col_count = mesh.shape["row"], mesh.shape["col"]
    planes = row_count == 2 * col_count and col_count == 4
    return jax.shard_map(
        functools.partial(per_device, planes),
        mesh=mesh,
        in_specs=(P("row", "col"), P(None, ("col", "row"), None), P()),
        out_specs=P("row", "col"),
        check_vma=False,
    )
```
